128 devices in a mesh: dp: 32 (over z, y_hi, x), expert: 4 (over y_lo, core).
Axes of the slice: x: 4, y: 4 (y_hi: 2, y_lo: 2; y = y_hi * 2 + y_lo), z: 4, core: 2. Of those that a mesh axis runs over, the one named last changes fastest.
Arguments:
- acts: bfloat16 [4, 16384, 4096], P('expert', 'dp'), may hold values from -8 to 8
- cotangent: bfloat16 [4, 16384, 14336], P('expert', 'dp'), may hold values from -1 to 1
- basis: bfloat16 [4, 4096, 256], P('expert'), may hold values from -1 to 1, as said below
- first_moment: float32 [4, 256, 14336], P('expert', 'dp'), may hold values from -0.6 to 0.6
- second_moment: float32 [4, 256, 14336], P('expert', 'dp'), may hold values from 0.001 to 0.05
- step_count: int32 [1], replicated, may hold values from 1 to 20
Outputs:
- update: bfloat16 [4, 4096, 14336], P('expert', 'dp')
- new_first: float32 [4, 256, 14336], P('expert', 'dp')
- new_second: float32 [4, 256, 14336], P('expert', 'dp')
The draws below stay inside these ranges and needn't reach their ends.
Inputs may be any that keep to these rules, and one draw needn't show every extreme that they name: Each expert's basis has orthonormal columns.
All inputs are finite; a program needn't handle non-finite values.
Results may differ from the reference program's by a relative error of at most 0.0051.
Values may be sent and summed in bfloat16 or wider, within the bound.
A program may use at most 128 MiB of HBM per device.

```python
import math
import jax
import jax.numpy as jnp

D = 4096
FF = 14336
R = 256
EXPERTS = 4
TOKENS = 16384


def make_basis(key):
    raw = jax.random.normal(jax.random.fold_in(key, 7), (EXPERTS, D, R), jnp.float32)
    ortho, upper = jnp.linalg.qr(raw)
    return ortho


def draw_basis(key, part):
    return make_basis(key).astype(jnp.bfloat16)


def draw_acts(key, part):
    ortho = make_basis(key).astype(jnp.bfloat16).astype(jnp.float32)
    noise = jax.random.normal(jax.random.fold_in(key, 11), (EXPERTS, TOKENS, D), jnp.float32)
    coeffs = jax.random.normal(jax.random.fold_in(key, 13), (EXPERTS, TOKENS, R), jnp.float32)
    ranks = jnp.arange(R, dtype=jnp.float32) / R
    spread = 0.5 * jnp.power(jnp.float32(10.0), ranks)
    along = jnp.einsum('etr,edr->etd', coeffs * spread[None, None, :], ortho)
    return jnp.clip(noise + along, -8.0, 8.0).astype(jnp.bfloat16)


def draw_cotangent(key, part):
    rises = jnp.arange(TOKENS, dtype=jnp.float32) / TOKENS
    base = jax.random.truncated_normal(key, -4.0, 4.0, (EXPERTS, TOKENS, FF), jnp.float32)
    scales = jnp.power(jnp.float32(3.0), rises)
    values = base * scales[None, :, None] / jnp.sqrt(jnp.float32(TOKENS))
    return jnp.clip(values, -1.0, 1.0).astype(jnp.bfloat16)


def levels(own_key, shape, pieces, least, high):
    def one(position, blocks):
        heights = jax.random.uniform(jax.random.fold_in(jax.random.fold_in(own_key, 6), position), (blocks,), jnp.float32, least / len(pieces), high / len(pieces))
        return jnp.repeat(jnp.exp(heights), shape[position] // blocks).reshape((-1,) + (1,) * (len(shape) - position - 1))

    factor_of = one(*pieces[0])
    for cut in pieces[1:]:
        factor_of = factor_of * one(*cut)
    return factor_of


def gaussian(key, extent, width, most, pieces=(), kind=jnp.bfloat16):
    result = width * jax.random.normal(key, extent, jnp.float32)
    if pieces:
        result = result * levels(key, extent, pieces, -0.22, 0.18)
    return jnp.clip(result, -most, most).astype(kind)


def setup_inputs(seed: int = 0) -> dict:
    seeds = jax.random.split(jax.random.key(seed), 7)
    acts = draw_acts(jax.random.fold_in(seeds[6], 71), 0)
    cotangent = draw_cotangent(jax.random.fold_in(seeds[6], 71), 0)
    basis = draw_basis(jax.random.fold_in(seeds[6], 71), 0)
    first_moment = gaussian(seeds[3], (EXPERTS, R, FF), 0.1, 0.6, ((0, 4), (1, 32)), jnp.float32)
    second_moment = jnp.clip(jnp.exp(math.log(0.05) - 3.912023 * jax.random.uniform(seeds[4], (EXPERTS, R, FF), jnp.float32) ** levels(seeds[4], (EXPERTS, R, FF), ((0, 4), (1, 32)), -0.2, 0.2)), 0.001, 0.05)
    step_count = jax.random.randint(seeds[5], (1,), 1, 21).astype(jnp.int32)
    return dict(acts=acts, cotangent=cotangent, basis=basis, first_moment=first_moment, second_moment=second_moment, step_count=step_count)


def reference(acts, cotangent, basis, first_moment, second_moment, step_count):
    count = acts.shape[0]
    sums_list = []
    for index in range(count):
        reduced = jnp.dot(acts[index].astype(jnp.float32), basis[index].astype(jnp.float32), preferred_element_type=jnp.float32).astype(jnp.bfloat16)
        sums_list.append(jnp.dot(reduced.T.astype(jnp.float32), cotangent[index].astype(jnp.float32), preferred_element_type=jnp.float32))
    sums = jnp.stack(sums_list)
    total = jnp.sum(sums * sums)
    limit = 0.25 * jnp.sqrt(jnp.float32(count * R * FF))
    factor = jnp.minimum(jnp.float32(1.0), limit / jnp.sqrt(total + 1e-06))
    grad = sums * factor
    new_first = 0.9 * first_moment + 0.1 * grad
    new_second = 0.999 * second_moment + 0.001 * grad * grad
    steps = step_count[0].astype(jnp.float32)
    corr_one = 1.0 - jnp.power(jnp.float32(0.9), steps)
    corr_two = 1.0 - jnp.power(jnp.float32(0.999), steps)
    normed = (new_first / corr_one / (jnp.sqrt(new_second / corr_two) + 1e-08)).astype(jnp.bfloat16)
    updates = []
    for index in range(count):
        updates.append((0.25 * jnp.dot(basis[index].astype(jnp.float32), normed[index].astype(jnp.float32), preferred_element_type=jnp.float32)).astype(jnp.bfloat16))
    return (jnp.stack(updates), new_first, new_second)
```

```python
import jax
import jax.numpy as jnp
from jax import lax
from jax.sharding import Mesh
from jax.sharding import PartitionSpec as P

D = 4096
FF = 14336
R = 256
DP = ("dp_0", "dp_1", "dp_2")
DP_EXPERT = ("dp_0", "dp_1", "dp_2", "expert_0", "expert_1")
EXPERT = ("expert_0", "expert_1")


def reduced_to_own(blocks, axes, sequence):
    inside = blocks.shape[1:]
    blocks = blocks.reshape(*(lax.axis_size(a) for a in axes), *inside)
    blocks = jnp.moveaxis(blocks, sequence, range(len(axes))).reshape(-1, *inside)
    for k in sequence:
        blocks = lax.psum_scatter(blocks, axes[k], scatter_dimension=0, tiled=True)
    return blocks[0]


def cut_along(array, dim, size):
    before, after = (array.shape[:dim], array.shape[dim + 1 :])
    return jnp.moveaxis(array.reshape(*before, size, -1, *after), dim, 0)


def scatter_axes(array, axes, sequence, dim):
    size = lax.axis_size(axes)
    return reduced_to_own(cut_along(array, dim, size), axes, sequence)


def one_axis_at_a_time(array, axes):
    for axis in axes:
        array = lax.psum(array, axis)
    return array


def local(acts, cotangent, basis, first_moment, second_moment, step_count):
    local_experts = acts.shape[0]
    dp_index = lax.axis_index(DP)
    reduced = jnp.einsum("etd,edr->ert", acts, basis, preferred_element_type=jnp.float32).astype(
        jnp.bfloat16
    )
    shared = scatter_axes(
        jnp.einsum("ekt,etf->kef", reduced, cotangent, preferred_element_type=jnp.float32).astype(
            jnp.bfloat16
        ),
        DP,
        (0, 2, 1),
        0,
    )
    sums = jnp.transpose(shared, (1, 0, 2)).astype(jnp.float32)
    local_total = jnp.sum(sums * sums)
    total = lax.psum(local_total, DP_EXPERT)
    all_experts = local_experts * lax.axis_size(EXPERT)
    limit = 0.25 * jnp.sqrt(jnp.float32(all_experts * R * FF))
    factor = jnp.minimum(jnp.float32(1.0), limit / jnp.sqrt(total + 1e-06))
    grad = sums * factor
    new_first = 0.9 * first_moment + 0.1 * grad
    new_second = 0.999 * second_moment + 0.001 * grad * grad
    steps = step_count[0].astype(jnp.float32)
    corr_one = 1.0 - jnp.power(jnp.float32(0.9), steps)
    corr_two = 1.0 - jnp.power(jnp.float32(0.999), steps)
    normed = (new_first / corr_one / (jnp.sqrt(new_second / corr_two) + 1e-08)).astype(jnp.bfloat16)
    width_rows = D // lax.axis_size(DP)
    basis_rows = lax.dynamic_slice_in_dim(basis, dp_index * width_rows, width_rows, 1)
    gathered = lax.all_gather(normed, DP, axis=1, tiled=True)
    product = jnp.einsum("edk,ekf->edf", basis_rows, gathered, preferred_element_type=jnp.float32)
    update = (0.25 * product).astype(jnp.bfloat16)
    return (update, new_first, new_second)


def solution(mesh):
    split = Mesh(
        mesh.devices.reshape(4, 2, 4, 2, 2), ("dp_0", "dp_1", "dp_2", "expert_0", "expert_1")
    )
    return jax.shard_map(
        local,
        mesh=split,
        in_specs=(
            P(EXPERT, DP, None),
            P(EXPERT, DP, None),
            P(EXPERT, None, None),
            P(EXPERT, DP, None),
            P(EXPERT, DP, None),
            P(),
        ),
        out_specs=(P(EXPERT, DP, None), P(EXPERT, DP, None), P(EXPERT, DP, None)),
        check_vma=False,
    )
```

```python
import functools

import jax
import jax.numpy as jnp
from jax import lax
from jax.experimental import pallas as pl
from jax.experimental.pallas import tpu as pltpu
from jax.sharding import Mesh
from jax.sharding import PartitionSpec as P

AXES = ("dp_0", "dp_1", "dp_2", "expert_0", "expert_1")
DP = ("dp_0", "dp_1", "dp_2")
EXPERT = ("expert_0", "expert_1")
MESH_ID = pl.DeviceIdType.MESH
RING = 4
FLOWS = 4
F32 = jnp.float32
BF16 = jnp.bfloat16


def powers(base, steps):
    value = jnp.ones(steps.shape, F32)
    for bit in range(8):
        on = (steps // (2**bit)) % 2
        value = value * jnp.where(on == 1, jnp.full(steps.shape, base ** (2**bit), F32), 1.0)
    return value


def step_kernel(
    groups, strip, limit,
    step_ref, reduced_ref, cot_hbm, basis_hbm, first_hbm, second_hbm,
    update_hbm, new_first_hbm, new_second_hbm,
    cot, own, ra, rb, rc, mix, own2, ra2, rb2, rc2, mix2, ysend, yrecv, sums,
    first, second, rows, perm, gath, nsend, nrecv, out, acc, near, acc2, far,
    rs_recv, rsy_recv, ag_recv, agy_recv, send, ysem, cot_sem, in_sem, near_sem, near_send,
    far_sem, far_send, out_sem,
):
    z, h, x = lax.axis_index("dp_0"), lax.axis_index("dp_1"), lax.axis_index("dp_2")
    lo, core = lax.axis_index("expert_0"), lax.axis_index("expert_1")
    width = FLOWS * strip
    ff = groups * width
    nrow = rows.shape[0]

    def turn(p, k):
        return lax.rem(p + (k % RING), RING)

    def at(zz, xx):
        return (zz, h, xx, lo, core)

    def major(f):
        return z if f % 2 == 0 else x

    def minor(f):
        return x if f % 2 == 0 else z

    def along_major(f, k):
        return at(turn(z, k), x) if f % 2 == 0 else at(z, turn(x, k))

    def along_minor(f, k):
        return at(z, turn(x, k)) if f % 2 == 0 else at(turn(z, k), x)

    def sense(f):
        return 1 if f < 2 else -1

    def remote(src, dst, ssem, rsem, dev):
        return pltpu.make_async_remote_copy(
            src_ref=src, dst_ref=dst, send_sem=ssem, recv_sem=rsem, device_id=dev, device_id_type=MESH_ID
        )

    def arrived(ref, sem):
        pltpu.make_async_copy(ref, ref, sem).wait()

    plane = [at(turn(z, k // RING), turn(x, k % RING)) for k in range(1, RING * RING)]
    column = [
        (z, lax.rem(h + (k // 4), 2), x, lax.rem(lo + (k // 2) % 2, 2), lax.rem(core + k % 2, 2))
        for k in range(1, 8)
    ]
    partner = (z, 1 - h, x, lo, core)

    barrier = pltpu.get_barrier_semaphore()
    for dev in plane + column:
        pl.semaphore_signal(barrier, inc=1, device_id=dev, device_id_type=MESH_ID)

    def cot_copy(t):
        cols = pl.ds(pl.multiple_of(t * width, width), width)
        return pltpu.make_async_copy(cot_hbm.at[0, :, cols], cot.at[t % 3], cot_sem.at[t % 3])

    for t in range(min(2, groups)):
        cot_copy(t).start()
    dp_index = z * (2 * RING) + h * RING + x
    loads = [
        pltpu.make_async_copy(first_hbm.at[0], first, in_sem.at[0]),
        pltpu.make_async_copy(second_hbm.at[0], second, in_sem.at[1]),
        pltpu.make_async_copy(
            basis_hbm.at[0, pl.ds(pl.multiple_of(dp_index * nrow, nrow), nrow), :], rows, in_sem.at[2]
        ),
    ]
    for load in loads:
        load.start()
    acc[...] = jnp.zeros_like(acc)
    pl.semaphore_wait(barrier, len(plane) + len(column))

    @pl.loop(0, groups + 5)
    def _(t):
        @pl.when(t < groups)
        def _():
            @pl.when(t + 2 < groups)
            def _():
                cot_copy(t + 2).start()

            cot_copy(t).wait()
            for f in range(FLOWS):
                part = jnp.dot(
                    reduced_ref[...], cot[t % 3, :, f * strip : (f + 1) * strip], preferred_element_type=F32
                )
                for u in range(RING):
                    for v in range(RING):
                        zz, xx = (u, v) if f % 2 == 0 else (v, u)
                        r0 = zz * 64 + xx * 8
                        own[f, t, u, v * 16 : (v + 1) * 16, :] = jnp.concatenate(
                            [part[r0 : r0 + 8], part[r0 + 32 : r0 + 40]], axis=0
                        ).astype(BF16)
                d = sense(f)
                p = major(f)
                remote(
                    own.at[f, t, turn(p, 2)], rb.at[f, t], send.at[1], rs_recv.at[1, f, t], along_major(f, -d)
                ).start()
                remote(
                    own.at[f, t, turn(p, d)], ra.at[f, t], send.at[0], rs_recv.at[0, f, t], along_major(f, d)
                ).start()

        @pl.when(jnp.logical_and(t >= 1, t < groups + 1))
        def _():
            s = t - 1
            for f in range(FLOWS):
                d = sense(f)
                arrived(rb.at[f, s], rs_recv.at[1, f, s])
                mix[f, s] = (own[f, s, turn(major(f), -d)].astype(F32) + rb[f, s].astype(F32)).astype(BF16)
                remote(
                    mix.at[f, s], rc.at[f, s], send.at[2], rs_recv.at[2, f, s], along_major(f, -d)
                ).start()

        @pl.when(jnp.logical_and(t >= 2, t < groups + 2))
        def _():
            s = t - 2
            for f in range(FLOWS):
                d = sense(f)
                q = minor(f)
                arrived(ra.at[f, s], rs_recv.at[0, f, s])
                arrived(rc.at[f, s], rs_recv.at[2, f, s])
                whole = own[f, s, major(f)].astype(F32) + ra[f, s].astype(F32) + rc[f, s].astype(F32)
                for v in range(RING):
                    own2[f, s, v] = whole[v * 16 : (v + 1) * 16].astype(BF16)
                remote(
                    own2.at[f, s, turn(q, 2)], rb2.at[f, s], send.at[4], rs_recv.at[4, f, s], along_minor(f, -d)
                ).start()
                remote(
                    own2.at[f, s, turn(q, d)], ra2.at[f, s], send.at[3], rs_recv.at[3, f, s], along_minor(f, d)
                ).start()

        @pl.when(jnp.logical_and(t >= 3, t < groups + 3))
        def _():
            s = t - 3
            for f in range(FLOWS):
                d = sense(f)
                arrived(rb2.at[f, s], rs_recv.at[4, f, s])
                mix2[f, s] = (own2[f, s, turn(minor(f), -d)].astype(F32) + rb2[f, s].astype(F32)).astype(BF16)
                remote(
                    mix2.at[f, s], rc2.at[f, s], send.at[5], rs_recv.at[5, f, s], along_minor(f, -d)
                ).start()

        @pl.when(jnp.logical_and(t >= 4, t < groups + 4))
        def _():
            s = t - 4
            for f in range(FLOWS):
                arrived(ra2.at[f, s], rs_recv.at[3, f, s])
                arrived(rc2.at[f, s], rs_recv.at[5, f, s])
                whole = own2[f, s, minor(f)].astype(F32) + ra2[f, s].astype(F32) + rc2[f, s].astype(F32)
                low = h == 0
                sums[s, f * 8 : (f + 1) * 8, :] = jnp.where(low, whole[:8], whole[8:])
                other = jnp.where(low, whole[8:], whole[:8])
                if f % 2 == 0:
                    held = other
                else:
                    ysend[s, (f - 1) * 8 : (f + 1) * 8, :] = jnp.concatenate([held, other], axis=0).astype(BF16)
            remote(ysend.at[s], yrecv.at[s], ysem.at[0], rsy_recv.at[s], partner).start()

        @pl.when(t >= 5)
        def _():
            s = t - 5
            arrived(yrecv.at[s], rsy_recv.at[s])
            grad = sums[s] + yrecv[s].astype(F32)
            sums[s] = grad
            square = grad * grad
            piece = acc[...]
            for i in range(FLOWS):
                for j in range(strip // 128):
                    piece = piece + square[i * 8 : (i + 1) * 8, j * 128 : (j + 1) * 128]
            acc[...] = piece

    for k, dev in enumerate(plane):
        remote(acc, near.at[k], near_send.at[k], near_sem.at[k], dev).start()
    for load in loads:
        load.wait()
    for o in range(2):
        r = lax.broadcasted_iota(jnp.int32, (256, 256), 0)
        q = lax.broadcasted_iota(jnp.int32, (256, 256), 1)
        u, v = q // 64, (q // 16) % 4
        zz, xx = (u, v) if o == 0 else (v, u)
        place = zz * 64 + ((q // 8) % 2) * 32 + xx * 8 + q % 8
        one = jnp.where(place == r, 1.0, 0.0).astype(BF16)
        perm[o] = jnp.dot(rows[...], one, preferred_element_type=F32).astype(BF16)
    steps = jnp.full((8, 128), step_ref[0], jnp.int32)
    corr_one = 1.0 - powers(0.9, steps)
    corr_two = 1.0 - powers(0.999, steps)
    total = acc[...]
    for k in range(len(plane)):
        arrived(near.at[k], near_sem.at[k])
        total = total + near[k]
    acc2[...] = total
    for k, dev in enumerate(column):
        remote(acc2, far.at[k], far_send.at[k], far_sem.at[k], dev).start()
    for k in range(len(column)):
        arrived(far.at[k], far_sem.at[k])
        total = total + far[k]
    total = jnp.sum(jnp.sum(total, axis=1, keepdims=True), axis=0, keepdims=True)
    factor = jnp.minimum(1.0, limit / jnp.sqrt(total + 1e-06))
    inv_one = jnp.max(1.0 / corr_one, axis=(0, 1), keepdims=True)
    inv_two = jnp.max(1.0 / corr_two, axis=(0, 1), keepdims=True)

    @pl.loop(0, groups + 5)
    def _(t):
        @pl.when(t < groups)
        def _():
            for f in range(FLOWS):
                cols = pl.ds(pl.multiple_of(t * width + f * strip, strip), strip)
                grad = sums[t, f * 8 : (f + 1) * 8, :] * factor
                one = 0.9 * first[:, cols] + 0.1 * grad
                two = 0.999 * second[:, cols] + 0.001 * grad * grad
                first[:, cols] = one
                second[:, cols] = two
                normed = (one * inv_one) / (jnp.sqrt(two * inv_two) + 1e-08)
                if f % 2 == 0:
                    held = normed
                else:
                    nsend[t, (f - 1) * 8 : (f + 1) * 8, :] = jnp.concatenate([held, normed], axis=0).astype(BF16)
            remote(nsend.at[t], nrecv.at[t], ysem.at[1], agy_recv.at[t], partner).start()

        @pl.when(jnp.logical_and(t >= 1, t < groups + 1))
        def _():
            s = t - 1
            arrived(nrecv.at[s], agy_recv.at[s])
            low = h == 0
            mine, theirs = nsend[s].astype(F32), nrecv[s].astype(F32)
            top, bottom = jnp.where(low, mine, theirs), jnp.where(low, theirs, mine)
            for f in range(FLOWS):
                d = sense(f)
                u, v = major(f), minor(f)
                gath[f, s, u, v] = jnp.concatenate(
                    [top[f * 8 : (f + 1) * 8], bottom[f * 8 : (f + 1) * 8]], axis=0
                ).astype(BF16)
                block = gath.at[f, s, u, v]
                remote(block, block, send.at[7], ag_recv.at[1, f, s], along_minor(f, -d)).start()
                remote(block, block, send.at[6], ag_recv.at[0, f, s], along_minor(f, d)).start()

        @pl.when(jnp.logical_and(t >= 2, t < groups + 2))
        def _():
            s = t - 2
            for f in range(FLOWS):
                d = sense(f)
                block = gath.at[f, s, major(f), turn(minor(f), d)]
                arrived(block, ag_recv.at[1, f, s])
                remote(block, block, send.at[8], ag_recv.at[2, f, s], along_minor(f, -d)).start()

        @pl.when(jnp.logical_and(t >= 3, t < groups + 3))
        def _():
            s = t - 3
            for f in range(FLOWS):
                d = sense(f)
                u, v = major(f), minor(f)
                arrived(gath.at[f, s, u, turn(v, -d)], ag_recv.at[0, f, s])
                arrived(gath.at[f, s, u, turn(v, 2)], ag_recv.at[2, f, s])
                block = gath.at[f, s, u]
                remote(block, block, send.at[10], ag_recv.at[4, f, s], along_major(f, -d)).start()
                remote(block, block, send.at[9], ag_recv.at[3, f, s], along_major(f, d)).start()

        @pl.when(jnp.logical_and(t >= 4, t < groups + 4))
        def _():
            s = t - 4
            for f in range(FLOWS):
                d = sense(f)
                block = gath.at[f, s, turn(major(f), d)]
                arrived(block, ag_recv.at[4, f, s])
                remote(block, block, send.at[11], ag_recv.at[5, f, s], along_major(f, -d)).start()

        @pl.when(t >= 5)
        def _():
            s = t - 5
            for f in range(FLOWS):
                d = sense(f)
                u = major(f)
                arrived(gath.at[f, s, turn(u, -d)], ag_recv.at[3, f, s])
                arrived(gath.at[f, s, turn(u, 2)], ag_recv.at[5, f, s])
                product = jnp.dot(perm[f % 2], gath[f, s].reshape(256, strip), preferred_element_type=F32)
                out[s, :, f * strip : (f + 1) * strip] = (0.25 * product).astype(BF16)
            cols = pl.ds(pl.multiple_of(s * width, width), width)
            pltpu.make_async_copy(out.at[s], update_hbm.at[0, :, cols], out_sem.at[2, s]).start()

    stores = [
        pltpu.make_async_copy(first, new_first_hbm.at[0], out_sem.at[0, 0]),
        pltpu.make_async_copy(second, new_second_hbm.at[0], out_sem.at[1, 0]),
    ]
    for store in stores:
        store.start()
    for k in range(len(plane)):
        arrived(acc, near_send.at[k])
    for k in range(len(column)):
        arrived(acc2, far_send.at[k])
    for k in (0, 1, 2, 9, 10, 11):
        arrived(ra, send.at[k])
    for k in (3, 4, 5, 6, 7, 8):
        arrived(ra2, send.at[k])
    for k in range(2):
        arrived(yrecv, ysem.at[k])
    for s in range(groups):
        pltpu.make_async_copy(out.at[s], update_hbm.at[0, :, s * width : (s + 1) * width], out_sem.at[2, s]).wait()
    for store in stores:
        store.wait()


def fused(step_count, reduced, cotangent, basis, first, second, groups, total_entries):
    _, tokens, ff = cotangent.shape
    strip = ff // groups // FLOWS
    width = FLOWS * strip
    n_dp = 2 * RING * RING
    out_rows = basis.shape[1] // n_dp
    any_space = pl.BlockSpec(memory_space=pl.ANY)
    limit = 0.25 * total_entries**0.5
    dma = pltpu.SemaphoreType.DMA
    big = pltpu.VMEM((FLOWS, groups, 64, strip), BF16)
    small = pltpu.VMEM((FLOWS, groups, 16, strip), BF16)
    yshape = (groups, 32, strip)
    return pl.pallas_call(
        functools.partial(step_kernel, groups, strip, limit),
        out_shape=(
            jax.ShapeDtypeStruct((1, out_rows, ff), BF16),
            jax.ShapeDtypeStruct(first.shape, F32),
            jax.ShapeDtypeStruct(second.shape, F32),
        ),
        in_specs=[
            pl.BlockSpec(memory_space=pltpu.SMEM),
            pl.BlockSpec(memory_space=pltpu.VMEM),
            any_space, any_space, any_space, any_space,
        ],
        out_specs=(any_space, any_space, any_space),
        scratch_shapes=[
            pltpu.VMEM((3, tokens, width), BF16),
            pltpu.VMEM((FLOWS, groups, RING, 64, strip), BF16),
            big, big, big, big,
            pltpu.VMEM((FLOWS, groups, RING, 16, strip), BF16),
            small, small, small, small,
            pltpu.VMEM(yshape, BF16),
            pltpu.VMEM(yshape, BF16),
            pltpu.VMEM(yshape, F32),
            pltpu.VMEM((8, ff), F32),
            pltpu.VMEM((8, ff), F32),
            pltpu.VMEM((out_rows, 256), BF16),
            pltpu.VMEM((2, out_rows, 256), BF16),
            pltpu.VMEM((FLOWS, groups, RING, RING, 16, strip), BF16),
            pltpu.VMEM(yshape, BF16),
            pltpu.VMEM(yshape, BF16),
            pltpu.VMEM((groups, out_rows, width), BF16),
            pltpu.VMEM((8, 128), F32),
            pltpu.VMEM((15, 8, 128), F32),
            pltpu.VMEM((8, 128), F32),
            pltpu.VMEM((7, 8, 128), F32),
            dma((6, FLOWS, groups)),
            dma((groups,)),
            dma((6, FLOWS, groups)),
            dma((groups,)),
            dma((12,)),
            dma((2,)),
            dma((3,)),
            dma((3,)),
            dma((15,)),
            dma((15,)),
            dma((7,)),
            dma((7,)),
            dma((3, groups)),
        ],
        compiler_params=pltpu.CompilerParams(
            collective_id=0, has_side_effects=True, vmem_limit_bytes=63 * 1024 * 1024
        ),
        name="galore_step",
    )(step_count, reduced, cotangent, basis, first, second)


def make_local(groups, total_entries):
    def local(acts, cotangent, basis, first_moment, second_moment, step_count):
        reduced = jnp.einsum("td,dr->rt", acts[0], basis[0], preferred_element_type=F32).astype(BF16)
        return fused(step_count, reduced, cotangent, basis, first_moment, second_moment, groups, total_entries)

    return local


def solution(mesh, groups=7, total_entries=4 * 256 * 14336):
    split = Mesh(mesh.devices.reshape(4, 2, 4, 2, 2), AXES)
    return jax.shard_map(
        make_local(groups, total_entries),
        mesh=split,
        in_specs=(
            P(EXPERT, DP, None),
            P(EXPERT, DP, None),
            P(EXPERT, None, None),
            P(EXPERT, DP, None),
            P(EXPERT, DP, None),
            P(),
        ),
        out_specs=(P(EXPERT, DP, None), P(EXPERT, DP, None), P(EXPERT, DP, None)),
        check_vma=False,
    )
```

```python
import functools

import jax
import jax.numpy as jnp
from jax import lax
from jax.experimental import pallas as pl
from jax.experimental.pallas import tpu as pltpu
from jax.sharding import Mesh
from jax.sharding import PartitionSpec as P

AXES = ("dp_0", "dp_1", "dp_2", "expert_0", "expert_1")
DP = ("dp_0", "dp_1", "dp_2")
EXPERT = ("expert_0", "expert_1")
MESH_ID = pl.DeviceIdType.MESH
RING = 4
FLOWS = 4
F32 = jnp.float32
BF16 = jnp.bfloat16


def powers(base, steps):
    value = jnp.ones(steps.shape, F32)
    for bit in range(8):
        on = (steps // (2**bit)) % 2
        value = value * jnp.where(on == 1, jnp.full(steps.shape, base ** (2**bit), F32), 1.0)
    return value


def step_kernel(
    plain, strip, limit,
    step_ref, acts_hbm, cot_hbm, basis_hbm, first_hbm, second_hbm,
    update_hbm, new_first_hbm, new_second_hbm,
    acts, basis, total_acc, reduced, cot, ycot,
    own, ra, rb, rc, mix, own2, ra2, rb2, rc2, mix2, ysend, yrecv, sums,
    yown, ypass, ypart, ysums, first, second, perm, yperm, gath, nsend, nrecv, gpass, gpart, out, yout,
    acc, near, acc2, far,
    rs_recv, rsy_recv, ag_recv, agy_recv, send, ysem, pass_recv, part_recv, gpass_recv, gpart_recv, pass_send,
    cot_sem, ycot_sem, in_sem, near_sem, near_send, far_sem, far_send, out_sem,
):
    z, h, x = lax.axis_index("dp_0"), lax.axis_index("dp_1"), lax.axis_index("dp_2")
    lo, core = lax.axis_index("expert_0"), lax.axis_index("expert_1")
    width = FLOWS * strip
    pair = 2 * strip
    base = plain * width
    steps_all = plain + 1
    nrow = out.shape[1]
    dp_index = z * (2 * RING) + h * RING + x

    def turn(p, k):
        return lax.rem(p + (k % RING), RING)

    def at(zz, xx):
        return (zz, h, xx, lo, core)

    def major(f):
        return z if f % 2 == 0 else x

    def minor(f):
        return x if f % 2 == 0 else z

    def along_major(f, k):
        return at(turn(z, k), x) if f % 2 == 0 else at(z, turn(x, k))

    def along_minor(f, k):
        return at(z, turn(x, k)) if f % 2 == 0 else at(turn(z, k), x)

    def sense(f):
        return 1 if f < 2 else -1

    up = (z, lax.rem(h + lo, 2), x, 1 - lo, core)
    down = (z, lax.rem(h + 1 + lo, 2), x, 1 - lo, core)

    def along_y(f):
        return up if f < 2 else down

    def remote(src, dst, ssem, rsem, dev):
        return pltpu.make_async_remote_copy(
            src_ref=src, dst_ref=dst, send_sem=ssem, recv_sem=rsem, device_id=dev, device_id_type=MESH_ID
        )

    def arrived(ref, sem):
        pltpu.make_async_copy(ref, ref, sem).wait()

    plane = [at(turn(z, k // RING), turn(x, k % RING)) for k in range(1, RING * RING)]
    column = [
        (z, lax.rem(h + (k // 4), 2), x, lax.rem(lo + (k // 2) % 2, 2), lax.rem(core + k % 2, 2))
        for k in range(1, 8)
    ]
    partner = (z, 1 - h, x, lo, core)

    barrier = pltpu.get_barrier_semaphore()
    for dev in plane + column:
        pl.semaphore_signal(barrier, inc=1, device_id=dev, device_id_type=MESH_ID)

    def cot_copy(t):
        cols = pl.ds(pl.multiple_of(t * width, width), width)
        return pltpu.make_async_copy(cot_hbm.at[0, :, cols], cot.at[t % 3], cot_sem.at[t % 3])

    deep = acts.shape[0]
    kdim = acts.shape[2]
    first_loads = []
    for k in range(deep):
        span = pl.ds(k * kdim, kdim)
        first_loads.append(
            (
                pltpu.make_async_copy(acts_hbm.at[0, :, span], acts.at[k], in_sem.at[2 + 2 * k]),
                pltpu.make_async_copy(basis_hbm.at[0, span, :], basis.at[span, :], in_sem.at[3 + 2 * k]),
            )
        )
    for one, two in first_loads:
        two.start()
        one.start()
    cot_copy(0).start()
    ycot_copy = pltpu.make_async_copy(cot_hbm.at[0, :, base : base + FLOWS * pair], ycot, ycot_sem)
    ycot_copy.start()
    cot_copy(1).start()
    loads = [
        pltpu.make_async_copy(first_hbm.at[0], first, in_sem.at[0]),
        pltpu.make_async_copy(second_hbm.at[0], second, in_sem.at[1]),
    ]
    for load in loads:
        load.start()
    acc[...] = jnp.zeros_like(acc)
    for k, (one, two) in enumerate(first_loads):
        two.wait()
        one.wait()
        piece = jnp.dot(acts[k], basis[k * kdim : (k + 1) * kdim, :], preferred_element_type=F32)
        if k == 0:
            total_acc[...] = piece
        else:
            total_acc[...] += piece
    reduced[...] = total_acc[...].T.astype(BF16)
    pl.semaphore_wait(barrier, len(plane) + len(column))

    def send_major(f, t):
        d = sense(f)
        p = major(f)
        remote(own.at[f, t, turn(p, 2)], rb.at[f, t], send.at[1], rs_recv.at[1, f, t], along_major(f, -d)).start()
        remote(own.at[f, t, turn(p, d)], ra.at[f, t], send.at[0], rs_recv.at[0, f, t], along_major(f, d)).start()

    @pl.loop(0, plain + 5)
    def _(t):
        @pl.when(t < plain)
        def _():
            @pl.when(jnp.logical_and(t >= 1, t + 1 < plain))
            def _():
                cot_copy(t + 1).start()

            cot_copy(t).wait()
            for f in range(FLOWS):
                part = jnp.dot(
                    reduced[...], cot[t % 3, :, f * strip : (f + 1) * strip], preferred_element_type=F32
                )
                for u in range(RING):
                    for v in range(RING):
                        zz, xx = (u, v) if f % 2 == 0 else (v, u)
                        r0 = zz * 64 + xx * 8
                        own[f, t, u, v * 16 : (v + 1) * 16, :] = jnp.concatenate(
                            [part[r0 : r0 + 8], part[r0 + 32 : r0 + 40]], axis=0
                        ).astype(BF16)
                send_major(f, t)

        @pl.when(t == 0)
        def _():
            ycot_copy.wait()
            for f in (0, 2, 1, 3):
                part = jnp.dot(reduced[...], ycot[:, f * pair : (f + 1) * pair], preferred_element_type=F32)
                for u in range(RING):
                    for v in range(RING):
                        zz, xx = (u, v) if f % 2 == 0 else (v, u)
                        for y in range(2):
                            r0 = zz * 64 + y * 32 + xx * 8
                            yown[f, y, u, v * 16 : (v + 1) * 16, :] = jnp.concatenate(
                                [part[r0 : r0 + 8, :strip], part[r0 : r0 + 8, strip:]], axis=0
                            ).astype(BF16)
                remote(yown.at[f, 1 - h], ypass.at[f], pass_send.at[0], pass_recv.at[f], along_y(f)).start()

        @pl.when(t == plain)
        def _():
            for f in range(FLOWS):
                arrived(ypart.at[f], part_recv.at[f])
                for u in range(RING):
                    own[f, plain, u] = (yown[f, h, u].astype(F32) + ypart[f, u].astype(F32)).astype(BF16)
                send_major(f, plain)

        @pl.when(jnp.logical_and(t >= 1, t < steps_all + 1))
        def _():
            s = t - 1
            for f in range(FLOWS):
                d = sense(f)
                arrived(rb.at[f, s], rs_recv.at[1, f, s])
                mix[f, s] = (own[f, s, turn(major(f), -d)].astype(F32) + rb[f, s].astype(F32)).astype(BF16)
                remote(
                    mix.at[f, s], rc.at[f, s], send.at[2], rs_recv.at[2, f, s], along_major(f, -d)
                ).start()

        @pl.when(jnp.logical_and(t >= 2, t < steps_all + 2))
        def _():
            s = t - 2
            for f in range(FLOWS):
                d = sense(f)
                q = minor(f)
                arrived(ra.at[f, s], rs_recv.at[0, f, s])
                arrived(rc.at[f, s], rs_recv.at[2, f, s])
                whole = own[f, s, major(f)].astype(F32) + ra[f, s].astype(F32) + rc[f, s].astype(F32)
                for v in range(RING):
                    own2[f, s, v] = whole[v * 16 : (v + 1) * 16].astype(BF16)
                remote(
                    own2.at[f, s, turn(q, 2)], rb2.at[f, s], send.at[4], rs_recv.at[4, f, s], along_minor(f, -d)
                ).start()
                remote(
                    own2.at[f, s, turn(q, d)], ra2.at[f, s], send.at[3], rs_recv.at[3, f, s], along_minor(f, d)
                ).start()

        for turn_of, flows in ((1, (0, 2)), (2, (1, 3))):

            @pl.when(t == turn_of)
            def _():
                for f in flows:
                    arrived(ypass.at[f], pass_recv.at[f])
                    remote(ypass.at[f], ypart.at[f], pass_send.at[1], part_recv.at[f], along_y(f)).start()

        @pl.when(jnp.logical_and(t >= 3, t < steps_all + 3))
        def _():
            s = t - 3
            for f in range(FLOWS):
                d = sense(f)
                arrived(rb2.at[f, s], rs_recv.at[4, f, s])
                mix2[f, s] = (own2[f, s, turn(minor(f), -d)].astype(F32) + rb2[f, s].astype(F32)).astype(BF16)
                remote(
                    mix2.at[f, s], rc2.at[f, s], send.at[5], rs_recv.at[5, f, s], along_minor(f, -d)
                ).start()

        def last_two(f, s):
            arrived(ra2.at[f, s], rs_recv.at[3, f, s])
            arrived(rc2.at[f, s], rs_recv.at[5, f, s])
            return own2[f, s, minor(f)].astype(F32) + ra2[f, s].astype(F32) + rc2[f, s].astype(F32)

        def add_squares(value):
            square = value * value
            piece = acc[...]
            for i in range(value.shape[0] // 8):
                for j in range(strip // 128):
                    piece = piece + square[i * 8 : (i + 1) * 8, j * 128 : (j + 1) * 128]
            acc[...] = piece

        @pl.when(jnp.logical_and(t >= 5, t < plain + 5))
        def _():
            s = t - 5
            arrived(yrecv.at[s], rsy_recv.at[s])
            grad = sums[s] + yrecv[s].astype(F32)
            sums[s] = grad
            add_squares(grad)

        @pl.when(jnp.logical_and(t >= 4, t < plain + 4))
        def _():
            s = t - 4
            for f in range(FLOWS):
                whole = last_two(f, s)
                low = h == 0
                sums[s, f * 8 : (f + 1) * 8, :] = jnp.where(low, whole[:8], whole[8:])
                other = jnp.where(low, whole[8:], whole[:8])
                if f % 2 == 0:
                    held = other
                else:
                    ysend[s, (f - 1) * 8 : (f + 1) * 8, :] = jnp.concatenate([held, other], axis=0).astype(BF16)
            remote(ysend.at[s], yrecv.at[s], ysem.at[0], rsy_recv.at[s], partner).start()

        @pl.when(t == plain + 4)
        def _():
            for f in range(FLOWS):
                whole = last_two(f, plain)
                ysums[f] = whole
                add_squares(whole)

    for k, dev in enumerate(plane):
        remote(acc, near.at[k], near_send.at[k], near_sem.at[k], dev).start()
    for load in loads:
        load.wait()
    rows = basis[pl.ds(pl.multiple_of(dp_index * nrow, nrow), nrow), :]
    r = lax.broadcasted_iota(jnp.int32, (256, 256), 0)
    q = lax.broadcasted_iota(jnp.int32, (256, 256), 1)
    for o in range(2):
        u, v = q // 64, (q // 16) % 4
        zz, xx = (u, v) if o == 0 else (v, u)
        place = zz * 64 + xx * 8 + q % 8
        half = (q // 8) % 2
        one = jnp.where(place + 32 * half == r, 1.0, 0.0).astype(BF16)
        perm[o] = jnp.dot(rows, one, preferred_element_type=F32).astype(BF16)
        for away in range(2):
            y = lax.rem(h + away, 2)
            for j in range(2):
                hit = jnp.logical_and(place + 32 * y == r, half == j)
                one = jnp.where(hit, 1.0, 0.0).astype(BF16)
                yperm[o, away, j] = jnp.dot(rows, one, preferred_element_type=F32).astype(BF16)
    steps = jnp.full((8, 128), step_ref[0], jnp.int32)
    corr_one = 1.0 - powers(0.9, steps)
    corr_two = 1.0 - powers(0.999, steps)
    total = acc[...]
    for k in range(len(plane)):
        arrived(near.at[k], near_sem.at[k])
        total = total + near[k]
    acc2[...] = total
    for k, dev in enumerate(column):
        remote(acc2, far.at[k], far_send.at[k], far_sem.at[k], dev).start()
    for k in range(len(column)):
        arrived(far.at[k], far_sem.at[k])
        total = total + far[k]
    total = jnp.sum(jnp.sum(total, axis=1, keepdims=True), axis=0, keepdims=True)
    factor = jnp.minimum(1.0, limit / jnp.sqrt(total + 1e-06))
    inv_one = jnp.max(1.0 / corr_one, axis=(0, 1), keepdims=True)
    inv_two = jnp.max(1.0 / corr_two, axis=(0, 1), keepdims=True)

    def adam(cols, sums_now):
        grad = sums_now * factor
        one = 0.9 * first[:, cols] + 0.1 * grad
        two = 0.999 * second[:, cols] + 0.001 * grad * grad
        first[:, cols] = one
        second[:, cols] = two
        return (one * inv_one) / (jnp.sqrt(two * inv_two) + 1e-08)

    def send_minor(f, a):
        d = sense(f)
        block = gath.at[f, a, major(f), minor(f)]
        remote(block, block, send.at[7], ag_recv.at[1, f, a], along_minor(f, -d)).start()
        remote(block, block, send.at[6], ag_recv.at[0, f, a], along_minor(f, d)).start()

    def y_place(f, k):
        return turn(major(f), (0, sense(f), -sense(f), 2)[k])

    def y_out(f, k):
        place = y_place(f, k)
        remote(
            gath.at[f, 0, place], gpass.at[f, place], pass_send.at[2], gpass_recv.at[f, k], along_y(f)
        ).start()

    def y_relay(f, k):
        place = y_place(f, k)
        arrived(gpass.at[f, place], gpass_recv.at[f, k])
        remote(
            gpass.at[f, place], gpart.at[f, place], pass_send.at[3], gpart_recv.at[f, k], along_y(f)
        ).start()

    for f in range(FLOWS):
        top = adam(pl.ds(base + f * pair, strip), ysums[f, :8])
        bottom = adam(pl.ds(base + f * pair + strip, strip), ysums[f, 8:])
        gath[f, 0, major(f), minor(f)] = jnp.concatenate([top, bottom], axis=0).astype(BF16)
        send_minor(f, 0)

    @pl.loop(0, plain + 5)
    def _(t):
        @pl.when(t < plain)
        def _():
            for f in range(FLOWS):
                cols = pl.ds(pl.multiple_of(t * width + f * strip, strip), strip)
                normed = adam(cols, sums[t, f * 8 : (f + 1) * 8, :])
                if f % 2 == 0:
                    held = normed
                else:
                    nsend[t, (f - 1) * 8 : (f + 1) * 8, :] = jnp.concatenate([held, normed], axis=0).astype(BF16)
            remote(nsend.at[t], nrecv.at[t], ysem.at[1], agy_recv.at[t], partner).start()

        @pl.when(jnp.logical_and(t >= 1, t < plain + 1))
        def _():
            s = t - 1
            arrived(nrecv.at[s], agy_recv.at[s])
            low = h == 0
            mine, theirs = nsend[s].astype(F32), nrecv[s].astype(F32)
            top, bottom = jnp.where(low, mine, theirs), jnp.where(low, theirs, mine)
            for f in range(FLOWS):
                gath[f, t, major(f), minor(f)] = jnp.concatenate(
                    [top[f * 8 : (f + 1) * 8], bottom[f * 8 : (f + 1) * 8]], axis=0
                ).astype(BF16)
                send_minor(f, t)

        @pl.when(jnp.logical_and(t >= 1, t < steps_all + 1))
        def _():
            a = t - 1
            for f in range(FLOWS):
                d = sense(f)
                block = gath.at[f, a, major(f), turn(minor(f), d)]
                arrived(block, ag_recv.at[1, f, a])
                remote(block, block, send.at[8], ag_recv.at[2, f, a], along_minor(f, -d)).start()

        @pl.when(jnp.logical_and(t >= 2, t < steps_all + 2))
        def _():
            a = t - 2
            for f in range(FLOWS):
                d = sense(f)
                u, v = major(f), minor(f)
                arrived(gath.at[f, a, u, turn(v, -d)], ag_recv.at[0, f, a])
                arrived(gath.at[f, a, u, turn(v, 2)], ag_recv.at[2, f, a])
                block = gath.at[f, a, u]
                remote(block, block, send.at[10], ag_recv.at[4, f, a], along_major(f, -d)).start()
                remote(block, block, send.at[9], ag_recv.at[3, f, a], along_major(f, d)).start()

        @pl.when(t == 2)
        def _():
            for f in range(FLOWS):
                y_out(f, 0)

        @pl.when(jnp.logical_and(t >= 3, t < steps_all + 3))
        def _():
            a = t - 3
            for f in range(FLOWS):
                d = sense(f)
                block = gath.at[f, a, turn(major(f), d)]
                arrived(block, ag_recv.at[4, f, a])
                remote(block, block, send.at[11], ag_recv.at[5, f, a], along_major(f, -d)).start()

        @pl.when(t == 3)
        def _():
            for f in range(FLOWS):
                y_out(f, 1)
            for f in range(FLOWS):
                y_relay(f, 0)

        @pl.when(t >= 4)
        def _():
            a = t - 4
            for f in range(FLOWS):
                d = sense(f)
                u = major(f)
                arrived(gath.at[f, a, turn(u, -d)], ag_recv.at[3, f, a])
                arrived(gath.at[f, a, turn(u, 2)], ag_recv.at[5, f, a])

        @pl.when(t == 4)
        def _():
            for f in range(FLOWS):
                y_out(f, 2)
                y_out(f, 3)
            for f in range(FLOWS):
                y_relay(f, 1)

        @pl.when(t == 5)
        def _():
            for f in range(FLOWS):
                y_relay(f, 2)

        @pl.when(t == 6)
        def _():
            for f in range(FLOWS):
                y_relay(f, 3)

        @pl.when(t >= 5)
        def _():
            s = t - 5
            for f in range(FLOWS):
                product = jnp.dot(perm[f % 2], gath[f, t - 4].reshape(256, strip), preferred_element_type=F32)
                out[s, :, f * strip : (f + 1) * strip] = (0.25 * product).astype(BF16)
            cols = pl.ds(pl.multiple_of(s * width, width), width)
            pltpu.make_async_copy(out.at[s], update_hbm.at[0, :, cols], out_sem.at[2, s]).start()

    stores = [
        pltpu.make_async_copy(first, new_first_hbm.at[0], out_sem.at[0, 0]),
        pltpu.make_async_copy(second, new_second_hbm.at[0], out_sem.at[1, 0]),
    ]
    for store in stores:
        store.start()
    for f in range(FLOWS):
        for k in range(RING):
            arrived(gpart.at[f, y_place(f, k)], gpart_recv.at[f, k])
        mine, theirs = gath[f, 0].reshape(256, strip), gpart[f].reshape(256, strip)
        for j in range(2):
            product = jnp.dot(yperm[f % 2, 0, j], mine, preferred_element_type=F32)
            product = product + jnp.dot(yperm[f % 2, 1, j], theirs, preferred_element_type=F32)
            yout[f, :, j * strip : (j + 1) * strip] = (0.25 * product).astype(BF16)
        store = pltpu.make_async_copy(
            yout.at[f], update_hbm.at[0, :, base + f * pair : base + (f + 1) * pair], out_sem.at[1, 1 + f]
        )
        store.start()
        stores.append(store)
    for k in range(len(plane)):
        arrived(acc, near_send.at[k])
    for k in range(len(column)):
        arrived(acc2, far_send.at[k])
    for k in (0, 1, 2, 9, 10, 11):
        arrived(ra, send.at[k])
    for k in (3, 4, 5, 6, 7, 8):
        arrived(ra2, send.at[k])
    for k in range(2):
        arrived(yrecv, ysem.at[k])
    for k in range(4):
        arrived(ypart, pass_send.at[k])
    for s in range(plain):
        pltpu.make_async_copy(out.at[s], update_hbm.at[0, :, s * width : (s + 1) * width], out_sem.at[2, s]).wait()
    for store in stores:
        store.wait()


def fused(step_count, acts, cotangent, basis, first, second, total_entries):
    _, tokens, ff = cotangent.shape
    depth, rank = basis.shape[1:]
    plain = 5
    strip = ff // (FLOWS * (plain + 2))
    width = FLOWS * strip
    chunks = 4
    out_rows = depth // (2 * RING * RING)
    any_space = pl.BlockSpec(memory_space=pl.ANY)
    limit = 0.25 * total_entries**0.5
    dma = pltpu.SemaphoreType.DMA
    vmem = pltpu.VMEM
    steps_all = plain + 1
    big = vmem((FLOWS, steps_all, 64, strip), BF16)
    small = vmem((FLOWS, steps_all, 16, strip), BF16)
    yshape = (plain, 32, strip)
    half = vmem((FLOWS, RING, 64, strip), BF16)
    return pl.pallas_call(
        functools.partial(step_kernel, plain, strip, limit),
        out_shape=(
            jax.ShapeDtypeStruct((1, out_rows, ff), BF16),
            jax.ShapeDtypeStruct(first.shape, F32),
            jax.ShapeDtypeStruct(second.shape, F32),
        ),
        in_specs=[
            pl.BlockSpec(memory_space=pltpu.SMEM),
            any_space, any_space, any_space, any_space, any_space,
        ],
        out_specs=(any_space, any_space, any_space),
        scratch_shapes=[
            vmem((chunks, tokens, depth // chunks), BF16),
            vmem((depth, rank), BF16),
            vmem((tokens, rank), F32),
            vmem((rank, tokens), BF16),
            vmem((3, tokens, width), BF16),
            vmem((tokens, 2 * width), BF16),
            vmem((FLOWS, steps_all, RING, 64, strip), BF16),
            big, big, big, big,
            vmem((FLOWS, steps_all, RING, 16, strip), BF16),
            small, small, small, small,
            vmem(yshape, BF16),
            vmem(yshape, BF16),
            vmem(yshape, F32),
            vmem((FLOWS, 2, RING, 64, strip), BF16),
            half,
            half,
            vmem((FLOWS, 16, strip), F32),
            vmem((8, ff), F32),
            vmem((8, ff), F32),
            vmem((2, out_rows, rank), BF16),
            vmem((2, 2, 2, out_rows, rank), BF16),
            vmem((FLOWS, steps_all, RING, RING, 16, strip), BF16),
            vmem(yshape, BF16),
            vmem(yshape, BF16),
            vmem((FLOWS, RING, RING, 16, strip), BF16),
            vmem((FLOWS, RING, RING, 16, strip), BF16),
            vmem((plain, out_rows, width), BF16),
            vmem((FLOWS, out_rows, 2 * strip), BF16),
            vmem((8, 128), F32),
            vmem((15, 8, 128), F32),
            vmem((8, 128), F32),
            vmem((7, 8, 128), F32),
            dma((6, FLOWS, steps_all)),
            dma((plain,)),
            dma((6, FLOWS, steps_all)),
            dma((plain,)),
            dma((12,)),
            dma((2,)),
            dma((FLOWS,)),
            dma((FLOWS,)),
            dma((FLOWS, RING)),
            dma((FLOWS, RING)),
            dma((4,)),
            dma((3,)),
            dma,
            dma((2 + 2 * chunks,)),
            dma((15,)),
            dma((15,)),
            dma((7,)),
            dma((7,)),
            dma((3, max(plain, 1 + FLOWS))),
        ],
        compiler_params=pltpu.CompilerParams(
            collective_id=0, has_side_effects=True, vmem_limit_bytes=63 * 1024 * 1024
        ),
        name="galore_step",
    )(step_count, acts, cotangent, basis, first, second)


def make_local(total_entries):
    def local(acts, cotangent, basis, first_moment, second_moment, step_count):
        return fused(step_count, acts, cotangent, basis, first_moment, second_moment, total_entries)

    return local


def solution(mesh, total_entries=4 * 256 * 14336):
    split = Mesh(mesh.devices.reshape(4, 2, 4, 2, 2), AXES)
    return jax.shard_map(
        make_local(total_entries),
        mesh=split,
        in_specs=(
            P(EXPERT, DP, None),
            P(EXPERT, DP, None),
            P(EXPERT, None, None),
            P(EXPERT, DP, None),
            P(EXPERT, DP, None),
            P(),
        ),
        out_specs=(P(EXPERT, DP, None), P(EXPERT, DP, None), P(EXPERT, DP, None)),
        check_vma=False,
    )
```

```python
import functools

import jax
import jax.numpy as jnp
from jax import lax
from jax.experimental import pallas as pl
from jax.experimental.pallas import tpu as pltpu
from jax.sharding import Mesh
from jax.sharding import PartitionSpec as P

AXES = ("dp_0", "dp_1", "dp_2", "expert_0", "expert_1")
DP = ("dp_0", "dp_1", "dp_2")
EXPERT = ("expert_0", "expert_1")
MESH_ID = pl.DeviceIdType.MESH
RING = 4
FLOWS = 4
F32 = jnp.float32
BF16 = jnp.bfloat16


def powers(base, steps):
    value = jnp.ones(steps.shape, F32)
    for bit in range(8):
        on = (steps // (2**bit)) % 2
        value = value * jnp.where(on == 1, jnp.full(steps.shape, base ** (2**bit), F32), 1.0)
    return value


def step_kernel(
    plain, strip, limit,
    step_ref, acts_hbm, cot_hbm, basis_hbm, first_hbm, second_hbm,
    out, new_first, new_second,
    acts, basis, total_acc, reduced, cot, ycot,
    own, ra, rb, rc, mix, own2, ra2, rb2, rc2, mix2, ysend, yrecv, sums,
    yown, ypass, ypart, ysums, perm, yperm, gath, nsend, nrecv, gpass, gpart,
    acc, near, acc2, far,
    rs_recv, rsy_recv, ag_recv, agy_recv, send, ysem, pass_recv, part_recv, gpass_recv, gpart_recv, pass_send,
    cot_sem, ycot_sem, in_sem, near_sem, near_send, far_sem, far_send,
):
    z, h, x = lax.axis_index("dp_0"), lax.axis_index("dp_1"), lax.axis_index("dp_2")
    lo, core = lax.axis_index("expert_0"), lax.axis_index("expert_1")
    width = FLOWS * strip
    pair = 2 * strip
    base = plain * width
    steps_all = plain + 1
    nrow = out.shape[1]
    first, second = new_first.at[0], new_second.at[0]
    dp_index = z * (2 * RING) + h * RING + x

    def turn(p, k):
        return lax.rem(p + (k % RING), RING)

    def at(zz, xx):
        return (zz, h, xx, lo, core)

    def major(f):
        return z if f % 2 == 0 else x

    def minor(f):
        return x if f % 2 == 0 else z

    def along_major(f, k):
        return at(turn(z, k), x) if f % 2 == 0 else at(z, turn(x, k))

    def along_minor(f, k):
        return at(z, turn(x, k)) if f % 2 == 0 else at(turn(z, k), x)

    def sense(f):
        return 1 if f < 2 else -1

    up = (z, lax.rem(h + lo, 2), x, 1 - lo, core)
    down = (z, lax.rem(h + 1 + lo, 2), x, 1 - lo, core)

    def along_y(f):
        return up if f < 2 else down

    def remote(src, dst, ssem, rsem, dev):
        return pltpu.make_async_remote_copy(
            src_ref=src, dst_ref=dst, send_sem=ssem, recv_sem=rsem, device_id=dev, device_id_type=MESH_ID
        )

    def arrived(ref, sem):
        pltpu.make_async_copy(ref, ref, sem).wait()

    plane = [at(turn(z, k // RING), turn(x, k % RING)) for k in range(1, RING * RING)]
    column = [
        (z, lax.rem(h + (k // 4), 2), x, lax.rem(lo + (k // 2) % 2, 2), lax.rem(core + k % 2, 2))
        for k in range(1, 8)
    ]
    partner = (z, 1 - h, x, lo, core)

    barrier = pltpu.get_barrier_semaphore()
    for dev in plane + column:
        pl.semaphore_signal(barrier, inc=1, device_id=dev, device_id_type=MESH_ID)

    def cot_copy(t):
        cols = pl.ds(pl.multiple_of(t * width, width), width)
        return pltpu.make_async_copy(cot_hbm.at[0, :, cols], cot.at[t % 3], cot_sem.at[t % 3])

    deep = acts.shape[0]
    kdim = acts.shape[2]
    first_loads = []
    for k in range(deep):
        span = pl.ds(k * kdim, kdim)
        first_loads.append(
            (
                pltpu.make_async_copy(acts_hbm.at[0, :, span], acts.at[k], in_sem.at[2 + 2 * k]),
                pltpu.make_async_copy(basis_hbm.at[0, span, :], basis.at[span, :], in_sem.at[3 + 2 * k]),
            )
        )
    for one, two in first_loads:
        two.start()
        one.start()
    ycot_copy = pltpu.make_async_copy(cot_hbm.at[0, :, base : base + FLOWS * pair], ycot, ycot_sem)
    ycot_copy.start()
    cot_copy(0).start()
    cot_copy(1).start()
    loads = [
        pltpu.make_async_copy(first_hbm.at[0], first, in_sem.at[0]),
        pltpu.make_async_copy(second_hbm.at[0], second, in_sem.at[1]),
    ]
    for load in loads:
        load.start()
    acc[...] = jnp.zeros_like(acc)
    for k, (one, two) in enumerate(first_loads):
        two.wait()
        one.wait()
        piece = jnp.dot(acts[k], basis[k * kdim : (k + 1) * kdim, :], preferred_element_type=F32)
        if k == 0:
            total_acc[...] = piece
        else:
            total_acc[...] += piece
    reduced[...] = total_acc[...].T.astype(BF16)
    pl.semaphore_wait(barrier, len(plane) + len(column))

    def send_major(f, t):
        d = sense(f)
        p = major(f)
        remote(own.at[f, t, turn(p, 2)], rb.at[f, t], send.at[1], rs_recv.at[1, f, t], along_major(f, -d)).start()
        remote(own.at[f, t, turn(p, d)], ra.at[f, t], send.at[0], rs_recv.at[0, f, t], along_major(f, d)).start()

    @pl.loop(0, plain + 4)
    def _(t):
        def y_units(flows):
            for f in flows:
                part = jnp.dot(reduced[...], ycot[:, f * pair : (f + 1) * pair], preferred_element_type=F32)
                for u in range(RING):
                    for v in range(RING):
                        zz, xx = (u, v) if f % 2 == 0 else (v, u)
                        for y in range(2):
                            r0 = zz * 64 + y * 32 + xx * 8
                            yown[f, y, u, v * 16 : (v + 1) * 16, :] = jnp.concatenate(
                                [part[r0 : r0 + 8, :strip], part[r0 : r0 + 8, strip:]], axis=0
                            ).astype(BF16)
                remote(yown.at[f, 1 - h], ypass.at[f], pass_send.at[0], pass_recv.at[f], along_y(f)).start()

        @pl.when(t == 0)
        def _():
            ycot_copy.wait()
            y_units((0, 2))

        @pl.when(t < plain)
        def _():
            @pl.when(jnp.logical_and(t >= 1, t + 1 < plain))
            def _():
                cot_copy(t + 1).start()

            cot_copy(t).wait()
            for f in range(FLOWS):
                part = jnp.dot(
                    reduced[...], cot[t % 3, :, f * strip : (f + 1) * strip], preferred_element_type=F32
                )
                for u in range(RING):
                    for v in range(RING):
                        zz, xx = (u, v) if f % 2 == 0 else (v, u)
                        r0 = zz * 64 + xx * 8
                        own[f, t, u, v * 16 : (v + 1) * 16, :] = jnp.concatenate(
                            [part[r0 : r0 + 8], part[r0 + 32 : r0 + 40]], axis=0
                        ).astype(BF16)
                send_major(f, t)

        @pl.when(t == plain)
        def _():
            for f in range(FLOWS):
                arrived(ypart.at[f], part_recv.at[f])
                for u in range(RING):
                    own[f, plain, u] = (yown[f, h, u].astype(F32) + ypart[f, u].astype(F32)).astype(BF16)
                send_major(f, plain)

        @pl.when(jnp.logical_and(t >= 1, t < steps_all + 1))
        def _():
            s = t - 1
            for f in range(FLOWS):
                d = sense(f)
                arrived(rb.at[f, s], rs_recv.at[1, f, s])
                mix[f, s] = (own[f, s, turn(major(f), -d)].astype(F32) + rb[f, s].astype(F32)).astype(BF16)
                remote(
                    mix.at[f, s], rc.at[f, s], send.at[2], rs_recv.at[2, f, s], along_major(f, -d)
                ).start()

        @pl.when(jnp.logical_and(t >= 2, t < steps_all + 2))
        def _():
            s = t - 2
            for f in range(FLOWS):
                d = sense(f)
                q = minor(f)
                arrived(ra.at[f, s], rs_recv.at[0, f, s])
                arrived(rc.at[f, s], rs_recv.at[2, f, s])
                whole = own[f, s, major(f)].astype(F32) + ra[f, s].astype(F32) + rc[f, s].astype(F32)
                for v in range(RING):
                    own2[f, s, v] = whole[v * 16 : (v + 1) * 16].astype(BF16)

                @pl.when(s == plain)
                def _():
                    for k, away in ((5, 2), (4, -d)):
                        dst = (rb2 if k == 4 else rc2).at[f, plain]
                        remote(
                            own2.at[f, plain, turn(q, away)], dst, send.at[k], rs_recv.at[k, f, plain], along_minor(f, away)
                        ).start()

                @pl.when(s < plain)
                def _():
                    remote(
                        own2.at[f, s, turn(q, 2)], rb2.at[f, s], send.at[4], rs_recv.at[4, f, s], along_minor(f, -d)
                    ).start()

                remote(
                    own2.at[f, s, turn(q, d)], ra2.at[f, s], send.at[3], rs_recv.at[3, f, s], along_minor(f, d)
                ).start()

        @pl.when(t == 1)
        def _():
            y_units((1, 3))

        @pl.when(t == 3)
        def _():
            rows = basis[pl.ds(pl.multiple_of(dp_index * nrow, nrow), nrow), :]
            r = lax.broadcasted_iota(jnp.int32, (256, 256), 0)
            q = lax.broadcasted_iota(jnp.int32, (256, 256), 1)
            for o in range(2):
                u, v = q // 64, (q // 16) % 4
                zz, xx = (u, v) if o == 0 else (v, u)
                place = zz * 64 + xx * 8 + q % 8
                half = (q // 8) % 2
                one = jnp.where(place + 32 * half == r, 1.0, 0.0).astype(BF16)
                perm[o] = jnp.dot(rows, one, preferred_element_type=F32).astype(BF16)
                for away in range(2):
                    y = lax.rem(h + away, 2)
                    for j in range(2):
                        hit = jnp.logical_and(place + 32 * y == r, half == j)
                        one = jnp.where(hit, 1.0, 0.0).astype(BF16)
                        yperm[o, away, j] = jnp.dot(rows, one, preferred_element_type=F32).astype(BF16)

        for turn_of, flows in ((2, (0, 2)), (3, (1, 3))):

            @pl.when(t == turn_of)
            def _():
                for f in flows:
                    arrived(ypass.at[f], pass_recv.at[f])
                    remote(ypass.at[f], ypart.at[f], pass_send.at[1], part_recv.at[f], along_y(f)).start()

        @pl.when(jnp.logical_and(t >= 3, t < plain + 3))
        def _():
            s = t - 3
            for f in range(FLOWS):
                d = sense(f)
                arrived(rb2.at[f, s], rs_recv.at[4, f, s])
                mix2[f, s] = (own2[f, s, turn(minor(f), -d)].astype(F32) + rb2[f, s].astype(F32)).astype(BF16)
                remote(
                    mix2.at[f, s], rc2.at[f, s], send.at[5], rs_recv.at[5, f, s], along_minor(f, -d)
                ).start()

        def last_two(f, s):
            arrived(ra2.at[f, s], rs_recv.at[3, f, s])
            arrived(rc2.at[f, s], rs_recv.at[5, f, s])
            return own2[f, s, minor(f)].astype(F32) + ra2[f, s].astype(F32) + rc2[f, s].astype(F32)

        def add_squares(value):
            square = value * value
            piece = acc[...]
            for i in range(value.shape[0] // 8):
                for j in range(strip // 128):
                    piece = piece + square[i * 8 : (i + 1) * 8, j * 128 : (j + 1) * 128]
            acc[...] = piece

        @pl.when(jnp.logical_and(t >= 4, t < plain + 4))
        def _():
            s = t - 4
            for f in range(FLOWS):
                whole = last_two(f, s)
                low = h == 0
                sums[s, f * 8 : (f + 1) * 8, :] = jnp.where(low, whole[:8], whole[8:])
                other = jnp.where(low, whole[8:], whole[:8])
                if f % 2 == 0:
                    held = other
                else:
                    ysend[s, (f - 1) * 8 : (f + 1) * 8, :] = jnp.concatenate([held, other], axis=0).astype(BF16)

        def y_send(s):
            remote(ysend.at[s], yrecv.at[s], ysem.at[0], rsy_recv.at[s], partner).start()

        def y_take(s):
            arrived(yrecv.at[s], rsy_recv.at[s])
            grad = sums[s] + yrecv[s].astype(F32)
            sums[s] = grad
            add_squares(grad)

        @pl.when(t == plain + 1)
        def _():
            for s in range(plain - 2):
                y_send(s)

        @pl.when(t == plain + 2)
        def _():
            y_send(plain - 2)

        @pl.when(t == plain + 3)
        def _():
            y_send(plain - 1)
            for s in range(plain - 1):
                y_take(s)
            for f in range(FLOWS):
                arrived(rb2.at[f, plain], rs_recv.at[4, f, plain])
                whole = last_two(f, plain) + rb2[f, plain].astype(F32)
                ysums[f] = whole
                add_squares(whole)
            y_take(plain - 1)

    for k, dev in enumerate(plane):
        remote(acc, near.at[k], near_send.at[k], near_sem.at[k], dev).start()
    for load in loads:
        load.wait()
    steps = jnp.full((8, 128), step_ref[0], jnp.int32)
    corr_one = 1.0 - powers(0.9, steps)
    corr_two = 1.0 - powers(0.999, steps)
    total = acc[...]
    for k in range(len(plane)):
        arrived(near.at[k], near_sem.at[k])
        total = total + near[k]
    acc2[...] = total
    for k, dev in enumerate(column):
        remote(acc2, far.at[k], far_send.at[k], far_sem.at[k], dev).start()
    for k in range(len(column)):
        arrived(far.at[k], far_sem.at[k])
        total = total + far[k]
    total = jnp.sum(jnp.sum(total, axis=1, keepdims=True), axis=0, keepdims=True)
    factor = jnp.minimum(1.0, limit / jnp.sqrt(total + 1e-06))
    inv_one = jnp.max(1.0 / corr_one, axis=(0, 1), keepdims=True)
    inv_two = jnp.max(1.0 / corr_two, axis=(0, 1), keepdims=True)

    def adam(cols, sums_now):
        grad = sums_now * factor
        one = 0.9 * first[:, cols] + 0.1 * grad
        two = 0.999 * second[:, cols] + 0.001 * grad * grad
        first[:, cols] = one
        second[:, cols] = two
        return (one * inv_one) / (jnp.sqrt(two * inv_two) + 1e-08)

    def send_minor(f, a):
        d = sense(f)
        block = gath.at[f, a, major(f), minor(f)]
        remote(block, block, send.at[7], ag_recv.at[1, f, a], along_minor(f, -d)).start()
        remote(block, block, send.at[6], ag_recv.at[0, f, a], along_minor(f, d)).start()

    def y_place(f, k):
        return turn(major(f), (0, sense(f), -sense(f), 2)[k])

    def y_out(f, k):
        place = y_place(f, k)
        remote(
            gath.at[f, 0, place], gpass.at[f, place], pass_send.at[2], gpass_recv.at[f, k], along_y(f)
        ).start()

    def y_relay(f, k):
        place = y_place(f, k)
        arrived(gpass.at[f, place], gpass_recv.at[f, k])
        remote(
            gpass.at[f, place], gpart.at[f, place], pass_send.at[3], gpart_recv.at[f, k], along_y(f)
        ).start()

    for f in range(FLOWS):
        top = adam(pl.ds(base + f * pair, strip), ysums[f, :8])
        bottom = adam(pl.ds(base + f * pair + strip, strip), ysums[f, 8:])
        gath[f, 0, major(f), minor(f)] = jnp.concatenate([top, bottom], axis=0).astype(BF16)
        d = sense(f)
        block = gath.at[f, 0, major(f), minor(f)]
        for k, away in ((2, 2), (1, -d), (0, d)):
            remote(block, block, send.at[6 + k], ag_recv.at[k, f, 0], along_minor(f, away)).start()

    def send_block(f, a):
        d = sense(f)
        block = gath.at[f, a, major(f)]
        remote(block, block, send.at[10], ag_recv.at[4, f, a], along_major(f, -d)).start()
        remote(block, block, send.at[9], ag_recv.at[3, f, a], along_major(f, d)).start()

    def relay_block(f, a):
        d = sense(f)
        block = gath.at[f, a, turn(major(f), d)]
        arrived(block, ag_recv.at[4, f, a])
        remote(block, block, send.at[11], ag_recv.at[5, f, a], along_major(f, -d)).start()

    def take_block(f, a):
        d = sense(f)
        u = major(f)
        arrived(gath.at[f, a, turn(u, -d)], ag_recv.at[3, f, a])
        arrived(gath.at[f, a, turn(u, 2)], ag_recv.at[5, f, a])

    @pl.loop(0, plain + 5)
    def _(t):
        @pl.when(t < plain)
        def _():
            for f in range(FLOWS):
                cols = pl.ds(pl.multiple_of(t * width + f * strip, strip), strip)
                normed = adam(cols, sums[t, f * 8 : (f + 1) * 8, :])
                if f % 2 == 0:
                    held = normed
                else:
                    nsend[t, (f - 1) * 8 : (f + 1) * 8, :] = jnp.concatenate([held, normed], axis=0).astype(BF16)
            remote(nsend.at[t], nrecv.at[t], ysem.at[1], agy_recv.at[t], partner).start()

        @pl.when(jnp.logical_and(t >= 1, t < plain + 1))
        def _():
            s = t - 1
            arrived(nrecv.at[s], agy_recv.at[s])
            low = h == 0
            mine, theirs = nsend[s].astype(F32), nrecv[s].astype(F32)
            top, bottom = jnp.where(low, mine, theirs), jnp.where(low, theirs, mine)
            for f in range(FLOWS):
                gath[f, t, major(f), minor(f)] = jnp.concatenate(
                    [top[f * 8 : (f + 1) * 8], bottom[f * 8 : (f + 1) * 8]], axis=0
                ).astype(BF16)
                send_minor(f, t)

        @pl.when(t == 1)
        def _():
            for f in range(FLOWS):
                for k, away in ((0, -sense(f)), (1, sense(f)), (2, 2)):
                    arrived(gath.at[f, 0, major(f), turn(minor(f), away)], ag_recv.at[k, f, 0])
                send_block(f, 0)
            for f in range(FLOWS):
                y_out(f, 0)

        @pl.when(t == 2)
        def _():
            for f in range(FLOWS):
                relay_block(f, 0)
            for f in range(FLOWS):
                y_out(f, 1)

        @pl.when(jnp.logical_and(t >= 2, t < steps_all + 1))
        def _():
            a = t - 1
            for f in range(FLOWS):
                d = sense(f)
                block = gath.at[f, a, major(f), turn(minor(f), d)]
                arrived(block, ag_recv.at[1, f, a])
                remote(block, block, send.at[8], ag_recv.at[2, f, a], along_minor(f, -d)).start()

        @pl.when(jnp.logical_and(t >= 3, t < steps_all + 2))
        def _():
            a = t - 2
            for f in range(FLOWS):
                d = sense(f)
                u, v = major(f), minor(f)
                arrived(gath.at[f, a, u, turn(v, -d)], ag_recv.at[0, f, a])
                arrived(gath.at[f, a, u, turn(v, 2)], ag_recv.at[2, f, a])
                send_block(f, a)

        @pl.when(jnp.logical_and(t >= 4, t < steps_all + 3))
        def _():
            for f in range(FLOWS):
                relay_block(f, t - 3)

        @pl.when(t == 3)
        def _():
            for f in range(FLOWS):
                take_block(f, 0)
                y_out(f, 2)
                y_out(f, 3)

        @pl.when(t >= 5)
        def _():
            for f in range(FLOWS):
                take_block(f, t - 4)

        @pl.when(t == 5)
        def _():
            for f in range(FLOWS):
                y_relay(f, 0)
                y_relay(f, 1)

        @pl.when(t == 6)
        def _():
            for f in range(FLOWS):
                y_relay(f, 2)
                y_relay(f, 3)

        @pl.when(t >= 5)
        def _():
            s = t - 5
            for f in range(FLOWS):
                product = jnp.dot(perm[f % 2], gath[f, t - 4].reshape(256, strip), preferred_element_type=F32)
                cols = pl.ds(pl.multiple_of(s * width + f * strip, strip), strip)
                out[0, :, cols] = (0.25 * product).astype(BF16)
    for f in range(FLOWS):
        for k in range(RING):
            arrived(gpart.at[f, y_place(f, k)], gpart_recv.at[f, k])
        mine, theirs = gath[f, 0].reshape(256, strip), gpart[f].reshape(256, strip)
        for j in range(2):
            product = jnp.dot(yperm[f % 2, 0, j], mine, preferred_element_type=F32)
            product = product + jnp.dot(yperm[f % 2, 1, j], theirs, preferred_element_type=F32)
            start = base + f * pair + j * strip
            out[0, :, start : start + strip] = (0.25 * product).astype(BF16)
    for k in range(len(plane)):
        arrived(acc, near_send.at[k])
    for k in range(len(column)):
        arrived(acc2, far_send.at[k])
    for k in (0, 1, 2, 9, 10, 11):
        arrived(ra, send.at[k])
    for k in (3, 4, 5, 6, 7, 8):
        arrived(ra2, send.at[k])
    for k in range(2):
        arrived(yrecv, ysem.at[k])
    for k in range(4):
        arrived(ypart, pass_send.at[k])


def fused(step_count, acts, cotangent, basis, first, second, total_entries):
    _, tokens, ff = cotangent.shape
    depth, rank = basis.shape[1:]
    plain = 5
    strip = ff // (FLOWS * (plain + 2))
    width = FLOWS * strip
    chunks = 4
    out_rows = depth // (2 * RING * RING)
    any_space = pl.BlockSpec(memory_space=pl.ANY)
    in_vmem = pl.BlockSpec(memory_space=pltpu.VMEM)
    limit = 0.25 * total_entries**0.5
    dma = pltpu.SemaphoreType.DMA
    vmem = pltpu.VMEM
    steps_all = plain + 1
    big = vmem((FLOWS, steps_all, 64, strip), BF16)
    small = vmem((FLOWS, steps_all, 16, strip), BF16)
    yshape = (plain, 32, strip)
    half = vmem((FLOWS, RING, 64, strip), BF16)
    return pl.pallas_call(
        functools.partial(step_kernel, plain, strip, limit),
        out_shape=(
            vmem((1, out_rows, ff), BF16),
            vmem((1, 8, ff), F32),
            vmem((1, 8, ff), F32),
        ),
        in_specs=[
            pl.BlockSpec(memory_space=pltpu.SMEM),
            any_space, any_space, any_space, any_space, any_space,
        ],
        out_specs=(in_vmem,) * 3,
        scratch_shapes=[
            vmem((chunks, tokens, depth // chunks), BF16),
            vmem((depth, rank), BF16),
            vmem((tokens, rank), F32),
            vmem((rank, tokens), BF16),
            vmem((3, tokens, width), BF16),
            vmem((tokens, 2 * width), BF16),
            vmem((FLOWS, steps_all, RING, 64, strip), BF16),
            big, big, big, big,
            vmem((FLOWS, steps_all, RING, 16, strip), BF16),
            small, small, small, small,
            vmem(yshape, BF16),
            vmem(yshape, BF16),
            vmem(yshape, F32),
            vmem((FLOWS, 2, RING, 64, strip), BF16),
            half,
            half,
            vmem((FLOWS, 16, strip), F32),
            vmem((2, out_rows, rank), BF16),
            vmem((2, 2, 2, out_rows, rank), BF16),
            vmem((FLOWS, steps_all, RING, RING, 16, strip), BF16),
            vmem(yshape, BF16),
            vmem(yshape, BF16),
            vmem((FLOWS, RING, RING, 16, strip), BF16),
            vmem((FLOWS, RING, RING, 16, strip), BF16),
            vmem((8, 128), F32),
            vmem((15, 8, 128), F32),
            vmem((8, 128), F32),
            vmem((7, 8, 128), F32),
            dma((6, FLOWS, steps_all)),
            dma((plain,)),
            dma((6, FLOWS, steps_all)),
            dma((plain,)),
            dma((12,)),
            dma((2,)),
            dma((FLOWS,)),
            dma((FLOWS,)),
            dma((FLOWS, RING)),
            dma((FLOWS, RING)),
            dma((4,)),
            dma((3,)),
            dma,
            dma((2 + 2 * chunks,)),
            dma((15,)),
            dma((15,)),
            dma((7,)),
            dma((7,)),
        ],
        compiler_params=pltpu.CompilerParams(
            collective_id=0, has_side_effects=True, vmem_limit_bytes=56 * 1024 * 1024
        ),
        name="galore_step",
    )(step_count, acts, cotangent, basis, first, second)


def make_local(total_entries):
    def local(acts, cotangent, basis, first_moment, second_moment, step_count):
        return fused(step_count, acts, cotangent, basis, first_moment, second_moment, total_entries)

    return local


def solution(mesh, total_entries=4 * 256 * 14336):
    split = Mesh(mesh.devices.reshape(4, 2, 4, 2, 2), AXES)
    return jax.shard_map(
        make_local(total_entries),
        mesh=split,
        in_specs=(
            P(EXPERT, DP, None),
            P(EXPERT, DP, None),
            P(EXPERT, None, None),
            P(EXPERT, DP, None),
            P(EXPERT, DP, None),
            P(),
        ),
        out_specs=(P(EXPERT, DP, None), P(EXPERT, DP, None), P(EXPERT, DP, None)),
        check_vma=False,
    )
```

```python
import functools

import jax
import jax.numpy as jnp
from jax import lax
from jax.experimental import pallas as pl
from jax.experimental.pallas import tpu as pltpu
from jax.sharding import Mesh
from jax.sharding import PartitionSpec as P

AXES = ("dp_0", "dp_1", "dp_2", "expert_0", "expert_1")
DP = ("dp_0", "dp_1", "dp_2")
EXPERT = ("expert_0", "expert_1")
MESH_ID = pl.DeviceIdType.MESH
RING = 4
FLOWS = 4
F32 = jnp.float32
BF16 = jnp.bfloat16


def powers(base, steps):
    value = jnp.ones(steps.shape, F32)
    for bit in range(8):
        on = (steps // (2**bit)) % 2
        value = value * jnp.where(on == 1, jnp.full(steps.shape, base ** (2**bit), F32), 1.0)
    return value


def step_kernel(
    plain, strip, limit,
    step_ref, acts_hbm, cot_hbm, basis_hbm, first_hbm, second_hbm,
    out, new_first, new_second,
    acts, basis, total_acc, reduced, cot, ycot,
    own, ra, rb, rc, mix, own2, ra2, rb2, rc2, mix2, ysend, yrecv, sums,
    yown, ypass, ypart, ysums, perm, yperm, gath, nsend, nrecv, gpass, gpart,
    acc, near, acc2, far,
    rs_recv, rsy_recv, ag_recv, agy_recv, send, ysem, pass_recv, part_recv, gpass_recv, gpart_recv, pass_send,
    cot_sem, ycot_sem, in_sem, near_sem, near_send, far_sem, far_send,
):
    z, h, x = lax.axis_index("dp_0"), lax.axis_index("dp_1"), lax.axis_index("dp_2")
    lo, core = lax.axis_index("expert_0"), lax.axis_index("expert_1")
    width = FLOWS * strip
    pair = 2 * strip
    base = plain * width
    steps_all = plain + 1
    nrow = out.shape[1]
    first, second = new_first.at[0], new_second.at[0]
    dp_index = z * (2 * RING) + h * RING + x

    def turn(p, k):
        return lax.rem(p + (k % RING), RING)

    def at(zz, xx):
        return (zz, h, xx, lo, core)

    def major(f):
        return z if f % 2 == 0 else x

    def minor(f):
        return x if f % 2 == 0 else z

    def along_major(f, k):
        return at(turn(z, k), x) if f % 2 == 0 else at(z, turn(x, k))

    def along_minor(f, k):
        return at(z, turn(x, k)) if f % 2 == 0 else at(turn(z, k), x)

    def sense(f):
        return 1 if f < 2 else -1

    up = (z, lax.rem(h + lo, 2), x, 1 - lo, core)
    down = (z, lax.rem(h + 1 + lo, 2), x, 1 - lo, core)

    def along_y(f):
        return up if f < 2 else down

    def remote(src, dst, ssem, rsem, dev):
        return pltpu.make_async_remote_copy(
            src_ref=src, dst_ref=dst, send_sem=ssem, recv_sem=rsem, device_id=dev, device_id_type=MESH_ID
        )

    def arrived(ref, sem):
        pltpu.make_async_copy(ref, ref, sem).wait()

    plane = [at(turn(z, k // RING), turn(x, k % RING)) for k in range(1, RING * RING)]
    column = [
        (z, lax.rem(h + (k // 4), 2), x, lax.rem(lo + (k // 2) % 2, 2), lax.rem(core + k % 2, 2))
        for k in range(1, 8)
    ]
    partner = (z, 1 - h, x, lo, core)

    barrier = pltpu.get_barrier_semaphore()
    for dev in plane + column:
        pl.semaphore_signal(barrier, inc=1, device_id=dev, device_id_type=MESH_ID)

    def cot_copy(t):
        cols = pl.ds(pl.multiple_of(t * width, width), width)
        return pltpu.make_async_copy(cot_hbm.at[0, :, cols], cot.at[t % 3], cot_sem.at[t % 3])

    deep = acts.shape[0]
    kdim = acts.shape[2]
    first_loads = []
    for k in range(deep):
        span = pl.ds(k * kdim, kdim)
        first_loads.append(
            (
                pltpu.make_async_copy(acts_hbm.at[0, :, span], acts.at[k], in_sem.at[2 + 2 * k]),
                pltpu.make_async_copy(basis_hbm.at[0, span, :], basis.at[span, :], in_sem.at[3 + 2 * k]),
            )
        )
    for one, two in first_loads:
        two.start()
        one.start()
    ycot_copy = pltpu.make_async_copy(cot_hbm.at[0, :, base : base + FLOWS * pair], ycot, ycot_sem)
    ycot_copy.start()
    cot_copy(0).start()
    cot_copy(1).start()
    loads = [
        pltpu.make_async_copy(first_hbm.at[0], first, in_sem.at[0]),
        pltpu.make_async_copy(second_hbm.at[0], second, in_sem.at[1]),
    ]
    for load in loads:
        load.start()
    acc[...] = jnp.zeros_like(acc)
    for k, (one, two) in enumerate(first_loads):
        two.wait()
        one.wait()
        piece = jnp.dot(acts[k], basis[k * kdim : (k + 1) * kdim, :], preferred_element_type=F32)
        if k == 0:
            total_acc[...] = piece
        else:
            total_acc[...] += piece
    reduced[...] = total_acc[...].T.astype(BF16)
    pl.semaphore_wait(barrier, len(plane) + len(column))

    def send_major(f, t):
        d = sense(f)
        p = major(f)
        remote(own.at[f, t, turn(p, 2)], rb.at[f, t], send.at[1], rs_recv.at[1, f, t], along_major(f, -d)).start()
        remote(own.at[f, t, turn(p, d)], ra.at[f, t], send.at[0], rs_recv.at[0, f, t], along_major(f, d)).start()

    @pl.loop(0, plain + 4)
    def _(t):
        def y_units(flows):
            for f in flows:
                part = jnp.dot(reduced[...], ycot[:, f * pair : (f + 1) * pair], preferred_element_type=F32)
                for u in range(RING):
                    for v in range(RING):
                        zz, xx = (u, v) if f % 2 == 0 else (v, u)
                        for y in range(2):
                            r0 = zz * 64 + y * 32 + xx * 8
                            yown[f, y, u, v * 16 : (v + 1) * 16, :] = jnp.concatenate(
                                [part[r0 : r0 + 8, :strip], part[r0 : r0 + 8, strip:]], axis=0
                            ).astype(BF16)
                remote(yown.at[f, 1 - h], ypass.at[f], pass_send.at[0], pass_recv.at[f], along_y(f)).start()

        @pl.when(t == 0)
        def _():
            ycot_copy.wait()
            y_units((0, 3))

        @pl.when(t < plain)
        def _():
            @pl.when(jnp.logical_and(t >= 1, t + 1 < plain))
            def _():
                cot_copy(t + 1).start()

            cot_copy(t).wait()
            for f in range(FLOWS):
                part = jnp.dot(
                    reduced[...], cot[t % 3, :, f * strip : (f + 1) * strip], preferred_element_type=F32
                )
                for u in range(RING):
                    for v in range(RING):
                        zz, xx = (u, v) if f % 2 == 0 else (v, u)
                        r0 = zz * 64 + xx * 8
                        own[f, t, u, v * 16 : (v + 1) * 16, :] = jnp.concatenate(
                            [part[r0 : r0 + 8], part[r0 + 32 : r0 + 40]], axis=0
                        ).astype(BF16)
                send_major(f, t)

        @pl.when(t == plain)
        def _():
            for f in (0, 3, 1, 2):
                arrived(ypart.at[f], part_recv.at[f])
                for u in range(RING):
                    own[f, plain, u] = (yown[f, h, u].astype(F32) + ypart[f, u].astype(F32)).astype(BF16)
                send_major(f, plain)

        for turn_of, flows in ((2, (0, 3)), (3, (1, 2))):

            @pl.when(t == turn_of)
            def _():
                for f in flows:
                    arrived(ypass.at[f], pass_recv.at[f])
                    remote(ypass.at[f], ypart.at[f], pass_send.at[1], part_recv.at[f], along_y(f)).start()

        @pl.when(jnp.logical_and(t >= 1, t < steps_all + 1))
        def _():
            s = t - 1
            for f in range(FLOWS):
                d = sense(f)
                arrived(rb.at[f, s], rs_recv.at[1, f, s])
                mix[f, s] = (own[f, s, turn(major(f), -d)].astype(F32) + rb[f, s].astype(F32)).astype(BF16)
                remote(
                    mix.at[f, s], rc.at[f, s], send.at[2], rs_recv.at[2, f, s], along_major(f, -d)
                ).start()

        @pl.when(jnp.logical_and(t >= 2, t < steps_all + 2))
        def _():
            s = t - 2
            for f in range(FLOWS):
                d = sense(f)
                q = minor(f)
                arrived(ra.at[f, s], rs_recv.at[0, f, s])
                arrived(rc.at[f, s], rs_recv.at[2, f, s])
                whole = own[f, s, major(f)].astype(F32) + ra[f, s].astype(F32) + rc[f, s].astype(F32)
                for v in range(RING):
                    own2[f, s, v] = whole[v * 16 : (v + 1) * 16].astype(BF16)

                @pl.when(s == plain)
                def _():
                    for k, away in ((5, 2), (4, -d)):
                        dst = (rb2 if k == 4 else rc2).at[f, plain]
                        remote(
                            own2.at[f, plain, turn(q, away)], dst, send.at[k], rs_recv.at[k, f, plain], along_minor(f, away)
                        ).start()

                @pl.when(s < plain)
                def _():
                    remote(
                        own2.at[f, s, turn(q, 2)], rb2.at[f, s], send.at[4], rs_recv.at[4, f, s], along_minor(f, -d)
                    ).start()

                remote(
                    own2.at[f, s, turn(q, d)], ra2.at[f, s], send.at[3], rs_recv.at[3, f, s], along_minor(f, d)
                ).start()

        @pl.when(t == 1)
        def _():
            y_units((1, 2))

        @pl.when(t == 3)
        def _():
            rows = basis[pl.ds(pl.multiple_of(dp_index * nrow, nrow), nrow), :]
            r = lax.broadcasted_iota(jnp.int32, (256, 256), 0)
            q = lax.broadcasted_iota(jnp.int32, (256, 256), 1)
            for o in range(2):
                u, v = q // 64, (q // 16) % 4
                zz, xx = (u, v) if o == 0 else (v, u)
                place = zz * 64 + xx * 8 + q % 8
                half = (q // 8) % 2
                one = jnp.where(place + 32 * half == r, 1.0, 0.0).astype(BF16)
                perm[o] = jnp.dot(rows, one, preferred_element_type=F32).astype(BF16)
                for away in range(2):
                    y = lax.rem(h + away, 2)
                    for j in range(2):
                        hit = jnp.logical_and(place + 32 * y == r, half == j)
                        one = jnp.where(hit, 1.0, 0.0).astype(BF16)
                        yperm[o, away, j] = jnp.dot(rows, one, preferred_element_type=F32).astype(BF16)

        @pl.when(jnp.logical_and(t >= 3, t < plain + 3))
        def _():
            s = t - 3
            for f in range(FLOWS):
                d = sense(f)
                arrived(rb2.at[f, s], rs_recv.at[4, f, s])
                mix2[f, s] = (own2[f, s, turn(minor(f), -d)].astype(F32) + rb2[f, s].astype(F32)).astype(BF16)
                remote(
                    mix2.at[f, s], rc2.at[f, s], send.at[5], rs_recv.at[5, f, s], along_minor(f, -d)
                ).start()

        def last_two(f, s):
            arrived(ra2.at[f, s], rs_recv.at[3, f, s])
            arrived(rc2.at[f, s], rs_recv.at[5, f, s])
            return own2[f, s, minor(f)].astype(F32) + ra2[f, s].astype(F32) + rc2[f, s].astype(F32)

        def add_squares(value):
            square = value * value
            piece = acc[...]
            for i in range(value.shape[0] // 8):
                for j in range(strip // 128):
                    piece = piece + square[i * 8 : (i + 1) * 8, j * 128 : (j + 1) * 128]
            acc[...] = piece

        @pl.when(jnp.logical_and(t >= 4, t < plain + 4))
        def _():
            s = t - 4
            for f in range(FLOWS):
                whole = last_two(f, s)
                low = h == 0
                sums[s, f * 8 : (f + 1) * 8, :] = jnp.where(low, whole[:8], whole[8:])
                other = jnp.where(low, whole[8:], whole[:8])
                if f % 2 == 0:
                    held = other
                else:
                    ysend[s, (f - 1) * 8 : (f + 1) * 8, :] = jnp.concatenate([held, other], axis=0).astype(BF16)

        def y_send(s):
            remote(ysend.at[s], yrecv.at[s], ysem.at[0], rsy_recv.at[s], partner).start()

        def y_take(s):
            arrived(yrecv.at[s], rsy_recv.at[s])
            grad = sums[s] + yrecv[s].astype(F32)
            sums[s] = grad
            add_squares(grad)

        @pl.when(t == plain + 1)
        def _():
            for s in range(plain - 2):
                y_send(s)

        @pl.when(t == plain + 2)
        def _():
            y_send(plain - 2)

        @pl.when(t == plain + 3)
        def _():
            y_send(plain - 1)
            for s in range(plain - 1):
                y_take(s)
            for f in range(FLOWS):
                arrived(rb2.at[f, plain], rs_recv.at[4, f, plain])
                whole = last_two(f, plain) + rb2[f, plain].astype(F32)
                ysums[f] = whole
                add_squares(whole)
            y_take(plain - 1)

    for k, dev in enumerate(plane):
        remote(acc, near.at[k], near_send.at[k], near_sem.at[k], dev).start()
    for load in loads:
        load.wait()
    steps = jnp.full((8, 128), step_ref[0], jnp.int32)
    corr_one = 1.0 - powers(0.9, steps)
    corr_two = 1.0 - powers(0.999, steps)
    total = acc[...]
    for k in range(len(plane)):
        arrived(near.at[k], near_sem.at[k])
        total = total + near[k]
    acc2[...] = total
    for k, dev in enumerate(column):
        remote(acc2, far.at[k], far_send.at[k], far_sem.at[k], dev).start()
    for k in range(len(column)):
        arrived(far.at[k], far_sem.at[k])
        total = total + far[k]
    total = jnp.sum(jnp.sum(total, axis=1, keepdims=True), axis=0, keepdims=True)
    factor = jnp.minimum(1.0, limit / jnp.sqrt(total + 1e-06))
    inv_one = jnp.max(1.0 / corr_one, axis=(0, 1), keepdims=True)
    inv_two = jnp.max(1.0 / corr_two, axis=(0, 1), keepdims=True)

    def adam(cols, sums_now):
        grad = sums_now * factor
        one = 0.9 * first[:, cols] + 0.1 * grad
        two = 0.999 * second[:, cols] + 0.001 * grad * grad
        first[:, cols] = one
        second[:, cols] = two
        return (one * inv_one) / (jnp.sqrt(two * inv_two) + 1e-08)

    def send_minor(f, a):
        d = sense(f)
        block = gath.at[f, a, major(f), minor(f)]
        remote(block, block, send.at[7], ag_recv.at[1, f, a], along_minor(f, -d)).start()
        remote(block, block, send.at[6], ag_recv.at[0, f, a], along_minor(f, d)).start()

    def y_place(f, k):
        return turn(major(f), (0, sense(f), -sense(f), 2)[k])

    def y_out(f, k):
        place = y_place(f, k)
        remote(
            gath.at[f, 0, place], gpass.at[f, place], pass_send.at[2], gpass_recv.at[f, k], along_y(f)
        ).start()

    def y_relay(f, k):
        place = y_place(f, k)
        arrived(gpass.at[f, place], gpass_recv.at[f, k])
        remote(
            gpass.at[f, place], gpart.at[f, place], pass_send.at[3], gpart_recv.at[f, k], along_y(f)
        ).start()

    for f in range(FLOWS):
        top = adam(pl.ds(base + f * pair, strip), ysums[f, :8])
        bottom = adam(pl.ds(base + f * pair + strip, strip), ysums[f, 8:])
        gath[f, 0, major(f), minor(f)] = jnp.concatenate([top, bottom], axis=0).astype(BF16)
        d = sense(f)
        block = gath.at[f, 0, major(f), minor(f)]
        for k, away in ((2, 2), (1, -d), (0, d)):
            remote(block, block, send.at[6 + k], ag_recv.at[k, f, 0], along_minor(f, away)).start()

    def send_block(f, a):
        d = sense(f)
        block = gath.at[f, a, major(f)]
        remote(block, block, send.at[10], ag_recv.at[4, f, a], along_major(f, -d)).start()
        remote(block, block, send.at[9], ag_recv.at[3, f, a], along_major(f, d)).start()

    def relay_block(f, a):
        d = sense(f)
        block = gath.at[f, a, turn(major(f), d)]
        arrived(block, ag_recv.at[4, f, a])
        remote(block, block, send.at[11], ag_recv.at[5, f, a], along_major(f, -d)).start()

    def take_block(f, a):
        d = sense(f)
        u = major(f)
        arrived(gath.at[f, a, turn(u, -d)], ag_recv.at[3, f, a])
        arrived(gath.at[f, a, turn(u, 2)], ag_recv.at[5, f, a])

    @pl.loop(0, plain + 5)
    def _(t):
        @pl.when(t < plain)
        def _():
            for f in range(FLOWS):
                cols = pl.ds(pl.multiple_of(t * width + f * strip, strip), strip)
                normed = adam(cols, sums[t, f * 8 : (f + 1) * 8, :])
                if f % 2 == 0:
                    held = normed
                else:
                    nsend[t, (f - 1) * 8 : (f + 1) * 8, :] = jnp.concatenate([held, normed], axis=0).astype(BF16)
            remote(nsend.at[t], nrecv.at[t], ysem.at[1], agy_recv.at[t], partner).start()

        @pl.when(jnp.logical_and(t >= 1, t < plain + 1))
        def _():
            s = t - 1
            arrived(nrecv.at[s], agy_recv.at[s])
            low = h == 0
            mine, theirs = nsend[s].astype(F32), nrecv[s].astype(F32)
            top, bottom = jnp.where(low, mine, theirs), jnp.where(low, theirs, mine)
            for f in range(FLOWS):
                gath[f, t, major(f), minor(f)] = jnp.concatenate(
                    [top[f * 8 : (f + 1) * 8], bottom[f * 8 : (f + 1) * 8]], axis=0
                ).astype(BF16)
                send_minor(f, t)

        @pl.when(t == 1)
        def _():
            for f in range(FLOWS):
                for k, away in ((0, -sense(f)), (1, sense(f)), (2, 2)):
                    arrived(gath.at[f, 0, major(f), turn(minor(f), away)], ag_recv.at[k, f, 0])
                send_block(f, 0)
            for f in range(FLOWS):
                y_out(f, 0)

        @pl.when(t == 2)
        def _():
            for f in range(FLOWS):
                relay_block(f, 0)
            for f in range(FLOWS):
                y_out(f, 1)

        @pl.when(jnp.logical_and(t >= 2, t < steps_all + 1))
        def _():
            a = t - 1
            for f in range(FLOWS):
                d = sense(f)
                block = gath.at[f, a, major(f), turn(minor(f), d)]
                arrived(block, ag_recv.at[1, f, a])
                remote(block, block, send.at[8], ag_recv.at[2, f, a], along_minor(f, -d)).start()

        @pl.when(jnp.logical_and(t >= 3, t < steps_all + 2))
        def _():
            a = t - 2
            for f in range(FLOWS):
                d = sense(f)
                u, v = major(f), minor(f)
                arrived(gath.at[f, a, u, turn(v, -d)], ag_recv.at[0, f, a])
                arrived(gath.at[f, a, u, turn(v, 2)], ag_recv.at[2, f, a])
                send_block(f, a)

        @pl.when(jnp.logical_and(t >= 4, t < steps_all + 3))
        def _():
            for f in range(FLOWS):
                relay_block(f, t - 3)

        @pl.when(t == 3)
        def _():
            for f in range(FLOWS):
                take_block(f, 0)
                y_out(f, 2)
                y_out(f, 3)

        @pl.when(t >= 5)
        def _():
            for f in range(FLOWS):
                take_block(f, t - 4)

        @pl.when(t == 5)
        def _():
            for f in range(FLOWS):
                y_relay(f, 0)
                y_relay(f, 1)

        @pl.when(t == 6)
        def _():
            for f in range(FLOWS):
                y_relay(f, 2)
                y_relay(f, 3)

        @pl.when(t >= 5)
        def _():
            s = t - 5
            for f in range(FLOWS):
                product = jnp.dot(perm[f % 2], gath[f, t - 4].reshape(256, strip), preferred_element_type=F32)
                cols = pl.ds(pl.multiple_of(s * width + f * strip, strip), strip)
                out[0, :, cols] = (0.25 * product).astype(BF16)

        @pl.when(t == plain + 3)
        def _():
            for f in range(FLOWS):
                for k in range(RING):
                    arrived(gpart.at[f, y_place(f, k)], gpart_recv.at[f, k])
                mine, theirs = gath[f, 0].reshape(256, strip), gpart[f].reshape(256, strip)
                for j in range(2):
                    product = jnp.dot(yperm[f % 2, 0, j], mine, preferred_element_type=F32)
                    product = product + jnp.dot(yperm[f % 2, 1, j], theirs, preferred_element_type=F32)
                    start = base + f * pair + j * strip
                    out[0, :, start : start + strip] = (0.25 * product).astype(BF16)

    for k in range(len(plane)):
        arrived(acc, near_send.at[k])
    for k in range(len(column)):
        arrived(acc2, far_send.at[k])
    for k in (0, 1, 2, 9, 10, 11):
        arrived(ra, send.at[k])
    for k in (3, 4, 5, 6, 7, 8):
        arrived(ra2, send.at[k])
    for k in range(2):
        arrived(yrecv, ysem.at[k])
    for k in range(4):
        arrived(ypart, pass_send.at[k])


def fused(step_count, acts, cotangent, basis, first, second, total_entries):
    _, tokens, ff = cotangent.shape
    depth, rank = basis.shape[1:]
    plain = 5
    strip = ff // (FLOWS * (plain + 2))
    width = FLOWS * strip
    chunks = 4
    out_rows = depth // (2 * RING * RING)
    any_space = pl.BlockSpec(memory_space=pl.ANY)
    in_vmem = pl.BlockSpec(memory_space=pltpu.VMEM)
    limit = 0.25 * total_entries**0.5
    dma = pltpu.SemaphoreType.DMA
    vmem = pltpu.VMEM
    steps_all = plain + 1
    big = vmem((FLOWS, steps_all, 64, strip), BF16)
    small = vmem((FLOWS, steps_all, 16, strip), BF16)
    yshape = (plain, 32, strip)
    half = vmem((FLOWS, RING, 64, strip), BF16)
    return pl.pallas_call(
        functools.partial(step_kernel, plain, strip, limit),
        out_shape=(
            vmem((1, out_rows, ff), BF16),
            vmem((1, 8, ff), F32),
            vmem((1, 8, ff), F32),
        ),
        in_specs=[
            pl.BlockSpec(memory_space=pltpu.SMEM),
            any_space, any_space, any_space, any_space, any_space,
        ],
        out_specs=(in_vmem,) * 3,
        scratch_shapes=[
            vmem((chunks, tokens, depth // chunks), BF16),
            vmem((depth, rank), BF16),
            vmem((tokens, rank), F32),
            vmem((rank, tokens), BF16),
            vmem((3, tokens, width), BF16),
            vmem((tokens, 2 * width), BF16),
            vmem((FLOWS, steps_all, RING, 64, strip), BF16),
            big, big, big, big,
            vmem((FLOWS, steps_all, RING, 16, strip), BF16),
            small, small, small, small,
            vmem(yshape, BF16),
            vmem(yshape, BF16),
            vmem(yshape, F32),
            vmem((FLOWS, 2, RING, 64, strip), BF16),
            half,
            half,
            vmem((FLOWS, 16, strip), F32),
            vmem((2, out_rows, rank), BF16),
            vmem((2, 2, 2, out_rows, rank), BF16),
            vmem((FLOWS, steps_all, RING, RING, 16, strip), BF16),
            vmem(yshape, BF16),
            vmem(yshape, BF16),
            vmem((FLOWS, RING, RING, 16, strip), BF16),
            vmem((FLOWS, RING, RING, 16, strip), BF16),
            vmem((8, 128), F32),
            vmem((15, 8, 128), F32),
            vmem((8, 128), F32),
            vmem((7, 8, 128), F32),
            dma((6, FLOWS, steps_all)),
            dma((plain,)),
            dma((6, FLOWS, steps_all)),
            dma((plain,)),
            dma((12,)),
            dma((2,)),
            dma((FLOWS,)),
            dma((FLOWS,)),
            dma((FLOWS, RING)),
            dma((FLOWS, RING)),
            dma((4,)),
            dma((3,)),
            dma,
            dma((2 + 2 * chunks,)),
            dma((15,)),
            dma((15,)),
            dma((7,)),
            dma((7,)),
        ],
        compiler_params=pltpu.CompilerParams(
            collective_id=0, has_side_effects=True, vmem_limit_bytes=56 * 1024 * 1024
        ),
        name="galore_step",
    )(step_count, acts, cotangent, basis, first, second)


def make_local(total_entries):
    def local(acts, cotangent, basis, first_moment, second_moment, step_count):
        return fused(step_count, acts, cotangent, basis, first_moment, second_moment, total_entries)

    return local


def solution(mesh, total_entries=4 * 256 * 14336):
    split = Mesh(mesh.devices.reshape(4, 2, 4, 2, 2), AXES)
    return jax.shard_map(
        make_local(total_entries),
        mesh=split,
        in_specs=(
            P(EXPERT, DP, None),
            P(EXPERT, DP, None),
            P(EXPERT, None, None),
            P(EXPERT, DP, None),
            P(EXPERT, DP, None),
            P(),
        ),
        out_specs=(P(EXPERT, DP, None), P(EXPERT, DP, None), P(EXPERT, DP, None)),
        check_vma=False,
    )
```

```python
import functools

import jax
import jax.numpy as jnp
from jax import lax
from jax.experimental import pallas as pl
from jax.experimental.pallas import tpu as pltpu
from jax.sharding import Mesh
from jax.sharding import PartitionSpec as P

AXES = ("dp_0", "dp_1", "dp_2", "expert_0", "expert_1")
DP = ("dp_0", "dp_1", "dp_2")
EXPERT = ("expert_0", "expert_1")
MESH_ID = pl.DeviceIdType.MESH
RING = 4
FLOWS = 4
F32 = jnp.float32
BF16 = jnp.bfloat16


def powers(base, steps):
    value = jnp.ones(steps.shape, F32)
    for bit in range(8):
        on = (steps // (2**bit)) % 2
        value = value * jnp.where(on == 1, jnp.full(steps.shape, base ** (2**bit), F32), 1.0)
    return value


def step_kernel(
    plain, strip, limit,
    step_ref, acts_hbm, cot_hbm, basis_hbm, first_hbm, second_hbm,
    out, new_first, new_second,
    acts, basis, total_acc, reduced, cot, ycot,
    own, ra, rb, rc, mix, own2, ra2, rb2, rc2, mix2, ysend, yrecv, sums,
    yown, ypass, ypart, ysums, perm, yperm, gath, nsend, nrecv, gpass, gpart,
    acc, near, acc2, far,
    rs_recv, rsy_recv, ag_recv, agy_recv, send, ysem, pass_recv, part_recv, gpass_recv, gpart_recv, pass_send,
    cot_sem, ycot_sem, in_sem, near_sem, near_send, far_sem, far_send,
):
    z, h, x = lax.axis_index("dp_0"), lax.axis_index("dp_1"), lax.axis_index("dp_2")
    lo, core = lax.axis_index("expert_0"), lax.axis_index("expert_1")
    width = FLOWS * strip
    pair = 2 * strip
    base = plain * width
    steps_all = plain + 1
    nrow = out.shape[1]
    first, second = new_first.at[0], new_second.at[0]
    dp_index = z * (2 * RING) + h * RING + x

    def turn(p, k):
        return lax.rem(p + (k % RING), RING)

    def at(zz, xx):
        return (zz, h, xx, lo, core)

    def major(f):
        return z if f % 2 == 0 else x

    def minor(f):
        return x if f % 2 == 0 else z

    def along_major(f, k):
        return at(turn(z, k), x) if f % 2 == 0 else at(z, turn(x, k))

    def along_minor(f, k):
        return at(z, turn(x, k)) if f % 2 == 0 else at(turn(z, k), x)

    def sense(f):
        return 1 if f < 2 else -1

    up = (z, lax.rem(h + lo, 2), x, 1 - lo, core)
    down = (z, lax.rem(h + 1 + lo, 2), x, 1 - lo, core)

    def along_y(f):
        return up if f < 2 else down

    def remote(src, dst, ssem, rsem, dev):
        return pltpu.make_async_remote_copy(
            src_ref=src, dst_ref=dst, send_sem=ssem, recv_sem=rsem, device_id=dev, device_id_type=MESH_ID
        )

    def arrived(ref, sem):
        pltpu.make_async_copy(ref, ref, sem).wait()

    plane = [at(turn(z, k // RING), turn(x, k % RING)) for k in range(1, RING * RING)]
    column = [
        (z, lax.rem(h + (k // 4), 2), x, lax.rem(lo + (k // 2) % 2, 2), lax.rem(core + k % 2, 2))
        for k in range(1, 8)
    ]
    partner = (z, 1 - h, x, lo, core)

    barrier = pltpu.get_barrier_semaphore()
    for dev in plane + column:
        pl.semaphore_signal(barrier, inc=1, device_id=dev, device_id_type=MESH_ID)

    def cot_copy(t):
        cols = pl.ds(pl.multiple_of(t * width, width), width)
        return pltpu.make_async_copy(cot_hbm.at[0, :, cols], cot.at[t % 3], cot_sem.at[t % 3])

    deep = acts.shape[0]
    kdim = acts.shape[2]
    first_loads = []
    for k in range(deep):
        span = pl.ds(k * kdim, kdim)
        first_loads.append(
            (
                pltpu.make_async_copy(acts_hbm.at[0, :, span], acts.at[k], in_sem.at[2 + 2 * k]),
                pltpu.make_async_copy(basis_hbm.at[0, span, :], basis.at[span, :], in_sem.at[3 + 2 * k]),
            )
        )
    for one, two in first_loads:
        two.start()
        one.start()
    ycot_copy = pltpu.make_async_copy(cot_hbm.at[0, :, base : base + FLOWS * pair], ycot, ycot_sem)
    ycot_copy.start()
    cot_copy(0).start()
    cot_copy(1).start()
    loads = [
        pltpu.make_async_copy(first_hbm.at[0], first, in_sem.at[0]),
        pltpu.make_async_copy(second_hbm.at[0], second, in_sem.at[1]),
    ]
    for load in loads:
        load.start()
    acc[...] = jnp.zeros_like(acc)
    for k, (one, two) in enumerate(first_loads):
        two.wait()
        one.wait()
        piece = jnp.dot(acts[k], basis[k * kdim : (k + 1) * kdim, :], preferred_element_type=F32)
        if k == 0:
            total_acc[...] = piece
        else:
            total_acc[...] += piece
    reduced[...] = total_acc[...].T.astype(BF16)
    pl.semaphore_wait(barrier, len(plane) + len(column))

    def send_major(f, t):
        d = sense(f)
        p = major(f)
        remote(own.at[f, t, turn(p, 2)], rb.at[f, t], send.at[1], rs_recv.at[1, f, t], along_major(f, -d)).start()
        remote(own.at[f, t, turn(p, d)], ra.at[f, t], send.at[0], rs_recv.at[0, f, t], along_major(f, d)).start()

    @pl.loop(0, plain + 4)
    def _(t):
        def y_units(flows):
            for f in flows:
                part = jnp.dot(reduced[...], ycot[:, f * pair : (f + 1) * pair], preferred_element_type=F32)
                for u in range(RING):
                    for v in range(RING):
                        zz, xx = (u, v) if f % 2 == 0 else (v, u)
                        for y in range(2):
                            r0 = zz * 64 + y * 32 + xx * 8
                            yown[f, y, u, v * 16 : (v + 1) * 16, :] = jnp.concatenate(
                                [part[r0 : r0 + 8, :strip], part[r0 : r0 + 8, strip:]], axis=0
                            ).astype(BF16)
                remote(yown.at[f, 1 - h], ypass.at[f], pass_send.at[0], pass_recv.at[f], along_y(f)).start()

        @pl.when(t == 0)
        def _():
            ycot_copy.wait()
            y_units((0, 3))

        @pl.when(t < plain)
        def _():
            @pl.when(jnp.logical_and(t >= 1, t + 1 < plain))
            def _():
                cot_copy(t + 1).start()

            cot_copy(t).wait()
            for f in range(FLOWS):
                part = jnp.dot(
                    reduced[...], cot[t % 3, :, f * strip : (f + 1) * strip], preferred_element_type=F32
                )
                for u in range(RING):
                    for v in range(RING):
                        zz, xx = (u, v) if f % 2 == 0 else (v, u)
                        r0 = zz * 64 + xx * 8
                        own[f, t, u, v * 16 : (v + 1) * 16, :] = jnp.concatenate(
                            [part[r0 : r0 + 8], part[r0 + 32 : r0 + 40]], axis=0
                        ).astype(BF16)
                send_major(f, t)

        @pl.when(t == plain)
        def _():
            for f in (0, 3, 1, 2):
                arrived(ypart.at[f], part_recv.at[f])
                for u in range(RING):
                    own[f, plain, u] = (yown[f, h, u].astype(F32) + ypart[f, u].astype(F32)).astype(BF16)
                send_major(f, plain)

        for turn_of, flows in ((2, (0, 3)), (3, (1, 2))):

            @pl.when(t == turn_of)
            def _():
                for f in flows:
                    arrived(ypass.at[f], pass_recv.at[f])
                    remote(ypass.at[f], ypart.at[f], pass_send.at[1], part_recv.at[f], along_y(f)).start()

        @pl.when(jnp.logical_and(t >= 1, t < steps_all + 1))
        def _():
            s = t - 1
            for f in range(FLOWS):
                d = sense(f)
                arrived(rb.at[f, s], rs_recv.at[1, f, s])
                mix[f, s] = (own[f, s, turn(major(f), -d)].astype(F32) + rb[f, s].astype(F32)).astype(BF16)
                remote(
                    mix.at[f, s], rc.at[f, s], send.at[2], rs_recv.at[2, f, s], along_major(f, -d)
                ).start()

        @pl.when(jnp.logical_and(t >= 2, t < steps_all + 2))
        def _():
            s = t - 2
            for f in range(FLOWS):
                d = sense(f)
                q = minor(f)
                arrived(ra.at[f, s], rs_recv.at[0, f, s])
                arrived(rc.at[f, s], rs_recv.at[2, f, s])
                whole = own[f, s, major(f)].astype(F32) + ra[f, s].astype(F32) + rc[f, s].astype(F32)
                for v in range(RING):
                    own2[f, s, v] = whole[v * 16 : (v + 1) * 16].astype(BF16)

                @pl.when(s >= plain - 1)
                def _():
                    for k, away in ((5, 2), (4, -d)):
                        dst = (rb2 if k == 4 else rc2).at[f, s]
                        remote(
                            own2.at[f, s, turn(q, away)], dst, send.at[k], rs_recv.at[k, f, s], along_minor(f, away)
                        ).start()

                @pl.when(s < plain - 1)
                def _():
                    remote(
                        own2.at[f, s, turn(q, 2)], rb2.at[f, s], send.at[4], rs_recv.at[4, f, s], along_minor(f, -d)
                    ).start()

                remote(
                    own2.at[f, s, turn(q, d)], ra2.at[f, s], send.at[3], rs_recv.at[3, f, s], along_minor(f, d)
                ).start()

        @pl.when(t == 1)
        def _():
            y_units((1, 2))

        @pl.when(t == 3)
        def _():
            rows = basis[pl.ds(pl.multiple_of(dp_index * nrow, nrow), nrow), :]
            r = lax.broadcasted_iota(jnp.int32, (256, 256), 0)
            q = lax.broadcasted_iota(jnp.int32, (256, 256), 1)
            for o in range(2):
                u, v = q // 64, (q // 16) % 4
                zz, xx = (u, v) if o == 0 else (v, u)
                place = zz * 64 + xx * 8 + q % 8
                half = (q // 8) % 2
                one = jnp.where(place + 32 * half == r, 1.0, 0.0).astype(BF16)
                perm[o] = jnp.dot(rows, one, preferred_element_type=F32).astype(BF16)
                for away in range(2):
                    y = lax.rem(h + away, 2)
                    for j in range(2):
                        hit = jnp.logical_and(place + 32 * y == r, half == j)
                        one = jnp.where(hit, 1.0, 0.0).astype(BF16)
                        yperm[o, away, j] = jnp.dot(rows, one, preferred_element_type=F32).astype(BF16)

        @pl.when(jnp.logical_and(t >= 3, t < plain + 2))
        def _():
            s = t - 3
            for f in range(FLOWS):
                d = sense(f)
                arrived(rb2.at[f, s], rs_recv.at[4, f, s])
                mix2[f, s] = (own2[f, s, turn(minor(f), -d)].astype(F32) + rb2[f, s].astype(F32)).astype(BF16)
                remote(
                    mix2.at[f, s], rc2.at[f, s], send.at[5], rs_recv.at[5, f, s], along_minor(f, -d)
                ).start()

        def last_two(f, s):
            arrived(ra2.at[f, s], rs_recv.at[3, f, s])
            arrived(rc2.at[f, s], rs_recv.at[5, f, s])
            return own2[f, s, minor(f)].astype(F32) + ra2[f, s].astype(F32) + rc2[f, s].astype(F32)

        def add_squares(value):
            square = value * value
            piece = acc[...]
            for i in range(value.shape[0] // 8):
                for j in range(strip // 128):
                    piece = piece + square[i * 8 : (i + 1) * 8, j * 128 : (j + 1) * 128]
            acc[...] = piece

        def last_three(f, s):
            arrived(rb2.at[f, s], rs_recv.at[4, f, s])
            return last_two(f, s) + rb2[f, s].astype(F32)

        def split_rows(s, take):
            for f in range(FLOWS):
                whole = take(f, s)
                low = h == 0
                sums[s, f * 8 : (f + 1) * 8, :] = jnp.where(low, whole[:8], whole[8:])
                other = jnp.where(low, whole[8:], whole[:8])
                if f % 2 == 0:
                    held = other
                else:
                    ysend[s, (f - 1) * 8 : (f + 1) * 8, :] = jnp.concatenate([held, other], axis=0).astype(BF16)

        @pl.when(jnp.logical_and(t >= 4, t < plain + 3))
        def _():
            split_rows(t - 4, last_two)

        def y_send(s):
            remote(ysend.at[s], yrecv.at[s], ysem.at[0], rsy_recv.at[s], partner).start()

        def y_take(s):
            arrived(yrecv.at[s], rsy_recv.at[s])
            grad = sums[s] + yrecv[s].astype(F32)
            sums[s] = grad
            add_squares(grad)

        @pl.when(t == plain + 1)
        def _():
            for s in range(plain - 2):
                y_send(s)

        @pl.when(t == plain + 2)
        def _():
            y_send(plain - 2)
            split_rows(plain - 1, last_three)
            y_send(plain - 1)

        @pl.when(t == plain + 3)
        def _():
            for s in range(plain - 1):
                y_take(s)
            for f in range(FLOWS):
                whole = last_three(f, plain)
                ysums[f] = whole
                add_squares(whole)
            y_take(plain - 1)

    for k, dev in enumerate(plane):
        remote(acc, near.at[k], near_send.at[k], near_sem.at[k], dev).start()
    for load in loads:
        load.wait()
    steps = jnp.full((8, 128), step_ref[0], jnp.int32)
    corr_one = 1.0 - powers(0.9, steps)
    corr_two = 1.0 - powers(0.999, steps)
    total = acc[...]
    for k in range(len(plane)):
        arrived(near.at[k], near_sem.at[k])
        total = total + near[k]
    acc2[...] = total
    for k, dev in enumerate(column):
        remote(acc2, far.at[k], far_send.at[k], far_sem.at[k], dev).start()
    for k in range(len(column)):
        arrived(far.at[k], far_sem.at[k])
        total = total + far[k]
    total = jnp.sum(jnp.sum(total, axis=1, keepdims=True), axis=0, keepdims=True)
    factor = jnp.minimum(1.0, limit / jnp.sqrt(total + 1e-06))
    inv_one = jnp.max(1.0 / corr_one, axis=(0, 1), keepdims=True)
    inv_two = jnp.max(1.0 / corr_two, axis=(0, 1), keepdims=True)

    def adam(cols, sums_now):
        grad = sums_now * factor
        one = 0.9 * first[:, cols] + 0.1 * grad
        two = 0.999 * second[:, cols] + 0.001 * grad * grad
        first[:, cols] = one
        second[:, cols] = two
        return (one * inv_one) / (jnp.sqrt(two * inv_two) + 1e-08)

    def send_minor(f, a):
        d = sense(f)
        block = gath.at[f, a, major(f), minor(f)]
        remote(block, block, send.at[7], ag_recv.at[1, f, a], along_minor(f, -d)).start()
        remote(block, block, send.at[6], ag_recv.at[0, f, a], along_minor(f, d)).start()

    def y_place(f, k):
        return turn(major(f), (0, sense(f), -sense(f), 2)[k])

    def y_out(f, k):
        place = y_place(f, k)
        remote(
            gath.at[f, 0, place], gpass.at[f, place], pass_send.at[2], gpass_recv.at[f, k], along_y(f)
        ).start()

    def y_relay(f, k):
        place = y_place(f, k)
        arrived(gpass.at[f, place], gpass_recv.at[f, k])
        remote(
            gpass.at[f, place], gpart.at[f, place], pass_send.at[3], gpart_recv.at[f, k], along_y(f)
        ).start()

    for f in range(FLOWS):
        top = adam(pl.ds(base + f * pair, strip), ysums[f, :8])
        bottom = adam(pl.ds(base + f * pair + strip, strip), ysums[f, 8:])
        gath[f, 0, major(f), minor(f)] = jnp.concatenate([top, bottom], axis=0).astype(BF16)
        d = sense(f)
        block = gath.at[f, 0, major(f), minor(f)]
        for k, away in ((2, 2), (1, -d), (0, d)):
            remote(block, block, send.at[6 + k], ag_recv.at[k, f, 0], along_minor(f, away)).start()

    def send_block(f, a):
        d = sense(f)
        block = gath.at[f, a, major(f)]
        remote(block, block, send.at[10], ag_recv.at[4, f, a], along_major(f, -d)).start()
        remote(block, block, send.at[9], ag_recv.at[3, f, a], along_major(f, d)).start()

    def relay_block(f, a):
        d = sense(f)
        block = gath.at[f, a, turn(major(f), d)]
        arrived(block, ag_recv.at[4, f, a])
        remote(block, block, send.at[11], ag_recv.at[5, f, a], along_major(f, -d)).start()

    def take_block(f, a):
        d = sense(f)
        u = major(f)
        arrived(gath.at[f, a, turn(u, -d)], ag_recv.at[3, f, a])
        arrived(gath.at[f, a, turn(u, 2)], ag_recv.at[5, f, a])

    @pl.loop(0, plain + 5)
    def _(t):
        @pl.when(t < plain)
        def _():
            for f in range(FLOWS):
                cols = pl.ds(pl.multiple_of(t * width + f * strip, strip), strip)
                normed = adam(cols, sums[t, f * 8 : (f + 1) * 8, :])
                if f % 2 == 0:
                    held = normed
                else:
                    nsend[t, (f - 1) * 8 : (f + 1) * 8, :] = jnp.concatenate([held, normed], axis=0).astype(BF16)
            remote(nsend.at[t], nrecv.at[t], ysem.at[1], agy_recv.at[t], partner).start()

        @pl.when(jnp.logical_and(t >= 1, t < plain + 1))
        def _():
            s = t - 1
            arrived(nrecv.at[s], agy_recv.at[s])
            low = h == 0
            mine, theirs = nsend[s].astype(F32), nrecv[s].astype(F32)
            top, bottom = jnp.where(low, mine, theirs), jnp.where(low, theirs, mine)
            for f in range(FLOWS):
                gath[f, t, major(f), minor(f)] = jnp.concatenate(
                    [top[f * 8 : (f + 1) * 8], bottom[f * 8 : (f + 1) * 8]], axis=0
                ).astype(BF16)
                send_minor(f, t)

        @pl.when(t == 1)
        def _():
            for f in range(FLOWS):
                for k, away in ((0, -sense(f)), (1, sense(f)), (2, 2)):
                    arrived(gath.at[f, 0, major(f), turn(minor(f), away)], ag_recv.at[k, f, 0])
                send_block(f, 0)
            for f in range(FLOWS):
                y_out(f, 0)

        @pl.when(t == 2)
        def _():
            for f in range(FLOWS):
                relay_block(f, 0)
            for f in range(FLOWS):
                y_out(f, 1)

        @pl.when(jnp.logical_and(t >= 2, t < steps_all + 1))
        def _():
            a = t - 1
            for f in range(FLOWS):
                d = sense(f)
                block = gath.at[f, a, major(f), turn(minor(f), d)]
                arrived(block, ag_recv.at[1, f, a])
                remote(block, block, send.at[8], ag_recv.at[2, f, a], along_minor(f, -d)).start()

        @pl.when(jnp.logical_and(t >= 3, t < steps_all + 2))
        def _():
            a = t - 2
            for f in range(FLOWS):
                d = sense(f)
                u, v = major(f), minor(f)
                arrived(gath.at[f, a, u, turn(v, -d)], ag_recv.at[0, f, a])
                arrived(gath.at[f, a, u, turn(v, 2)], ag_recv.at[2, f, a])
                send_block(f, a)

        @pl.when(jnp.logical_and(t >= 4, t < steps_all + 3))
        def _():
            for f in range(FLOWS):
                relay_block(f, t - 3)

        @pl.when(t == 3)
        def _():
            for f in range(FLOWS):
                take_block(f, 0)
                y_out(f, 2)
                y_out(f, 3)

        @pl.when(t >= 5)
        def _():
            for f in range(FLOWS):
                take_block(f, t - 4)

        @pl.when(t == 5)
        def _():
            for f in range(FLOWS):
                y_relay(f, 0)
                y_relay(f, 1)

        @pl.when(t == 6)
        def _():
            for f in range(FLOWS):
                y_relay(f, 2)
                y_relay(f, 3)

        @pl.when(t >= 5)
        def _():
            s = t - 5
            for f in range(FLOWS):
                product = jnp.dot(perm[f % 2], gath[f, t - 4].reshape(256, strip), preferred_element_type=F32)
                cols = pl.ds(pl.multiple_of(s * width + f * strip, strip), strip)
                out[0, :, cols] = (0.25 * product).astype(BF16)

        @pl.when(t == plain + 3)
        def _():
            for f in range(FLOWS):
                for k in range(RING):
                    arrived(gpart.at[f, y_place(f, k)], gpart_recv.at[f, k])
                mine, theirs = gath[f, 0].reshape(256, strip), gpart[f].reshape(256, strip)
                for j in range(2):
                    product = jnp.dot(yperm[f % 2, 0, j], mine, preferred_element_type=F32)
                    product = product + jnp.dot(yperm[f % 2, 1, j], theirs, preferred_element_type=F32)
                    start = base + f * pair + j * strip
                    out[0, :, start : start + strip] = (0.25 * product).astype(BF16)

    for k in range(len(plane)):
        arrived(acc, near_send.at[k])
    for k in range(len(column)):
        arrived(acc2, far_send.at[k])
    for k in (0, 1, 2, 9, 10, 11):
        arrived(ra, send.at[k])
    for k in (3, 4, 5, 6, 7, 8):
        arrived(ra2, send.at[k])
    for k in range(2):
        arrived(yrecv, ysem.at[k])
    for k in range(4):
        arrived(ypart, pass_send.at[k])


def fused(step_count, acts, cotangent, basis, first, second, total_entries):
    _, tokens, ff = cotangent.shape
    depth, rank = basis.shape[1:]
    plain = 5
    strip = ff // (FLOWS * (plain + 2))
    width = FLOWS * strip
    chunks = 4
    out_rows = depth // (2 * RING * RING)
    any_space = pl.BlockSpec(memory_space=pl.ANY)
    in_vmem = pl.BlockSpec(memory_space=pltpu.VMEM)
    limit = 0.25 * total_entries**0.5
    dma = pltpu.SemaphoreType.DMA
    vmem = pltpu.VMEM
    steps_all = plain + 1
    big = vmem((FLOWS, steps_all, 64, strip), BF16)
    small = vmem((FLOWS, steps_all, 16, strip), BF16)
    yshape = (plain, 32, strip)
    half = vmem((FLOWS, RING, 64, strip), BF16)
    return pl.pallas_call(
        functools.partial(step_kernel, plain, strip, limit),
        out_shape=(
            vmem((1, out_rows, ff), BF16),
            vmem((1, 8, ff), F32),
            vmem((1, 8, ff), F32),
        ),
        in_specs=[
            pl.BlockSpec(memory_space=pltpu.SMEM),
            any_space, any_space, any_space, any_space, any_space,
        ],
        out_specs=(in_vmem,) * 3,
        scratch_shapes=[
            vmem((chunks, tokens, depth // chunks), BF16),
            vmem((depth, rank), BF16),
            vmem((tokens, rank), F32),
            vmem((rank, tokens), BF16),
            vmem((3, tokens, width), BF16),
            vmem((tokens, 2 * width), BF16),
            vmem((FLOWS, steps_all, RING, 64, strip), BF16),
            big, big, big, big,
            vmem((FLOWS, steps_all, RING, 16, strip), BF16),
            small, small, small, small,
            vmem(yshape, BF16),
            vmem(yshape, BF16),
            vmem(yshape, F32),
            vmem((FLOWS, 2, RING, 64, strip), BF16),
            half,
            half,
            vmem((FLOWS, 16, strip), F32),
            vmem((2, out_rows, rank), BF16),
            vmem((2, 2, 2, out_rows, rank), BF16),
            vmem((FLOWS, steps_all, RING, RING, 16, strip), BF16),
            vmem(yshape, BF16),
            vmem(yshape, BF16),
            vmem((FLOWS, RING, RING, 16, strip), BF16),
            vmem((FLOWS, RING, RING, 16, strip), BF16),
            vmem((8, 128), F32),
            vmem((15, 8, 128), F32),
            vmem((8, 128), F32),
            vmem((7, 8, 128), F32),
            dma((6, FLOWS, steps_all)),
            dma((plain,)),
            dma((6, FLOWS, steps_all)),
            dma((plain,)),
            dma((12,)),
            dma((2,)),
            dma((FLOWS,)),
            dma((FLOWS,)),
            dma((FLOWS, RING)),
            dma((FLOWS, RING)),
            dma((4,)),
            dma((3,)),
            dma,
            dma((2 + 2 * chunks,)),
            dma((15,)),
            dma((15,)),
            dma((7,)),
            dma((7,)),
        ],
        compiler_params=pltpu.CompilerParams(
            collective_id=0, has_side_effects=True, vmem_limit_bytes=56 * 1024 * 1024
        ),
        name="galore_step",
    )(step_count, acts, cotangent, basis, first, second)


def make_local(total_entries):
    def local(acts, cotangent, basis, first_moment, second_moment, step_count):
        return fused(step_count, acts, cotangent, basis, first_moment, second_moment, total_entries)

    return local


def solution(mesh, total_entries=4 * 256 * 14336):
    split = Mesh(mesh.devices.reshape(4, 2, 4, 2, 2), AXES)
    return jax.shard_map(
        make_local(total_entries),
        mesh=split,
        in_specs=(
            P(EXPERT, DP, None),
            P(EXPERT, DP, None),
            P(EXPERT, None, None),
            P(EXPERT, DP, None),
            P(EXPERT, DP, None),
            P(),
        ),
        out_specs=(P(EXPERT, DP, None), P(EXPERT, DP, None), P(EXPERT, DP, None)),
        check_vma=False,
    )
```
